256 devices in a mesh: rows: 32 (over x_lo, z, core), cols: 8 (over x_hi, y).
Axes of the slice: x: 4 (x_hi: 2, x_lo: 2; x = x_hi * 2 + x_lo), y: 4, z: 8, core: 2. Of those that a mesh axis runs over, the one named last changes fastest.
Arguments:
- rhs: float32 [65536, 16], P(('rows', 'cols')), may hold values from -6 to 6
- diagonal: float32 [65536], P(('rows', 'cols')), may hold values from 1 to 16
- blocks: float32 [512, 16, 128, 128], P('rows', 'cols'), may hold values from -0.078125 to 0.078125
- block_cols: int32 [512, 16], P('rows', 'cols'), may hold values from 0 to 63
- counts: int32 [512, 8], P('rows', 'cols'), may hold values from 1 to 2
Outputs:
- solution: float32 [65536, 16], P(('rows', 'cols'))
The draws below stay inside these ranges and needn't reach their ends.
Inputs may be any that keep to these rules, and one draw needn't show every extreme that they name: Every entry of block_cols names a block column within its slot's group, from 0 to 63; entries may repeat within a row. `counts`: every count lies between 1 and 2; the slots past the count in a group hold blocks that are not used.
All inputs are finite; a program needn't handle non-finite values.
Results may differ from the reference program's by a relative error of at most 0.0001.
Values sent between devices are 32-bit elements; how exact they have to be, the bound alone decides.
No kernel may reach another device: no remote copies, remote signals or barrier semaphores. Data moves between devices by JAX's collectives and lax.ppermute only.
A program may use at most 64 MiB of HBM per device.

```python
import math
import jax
import jax.numpy as jnp
from jax import lax

BS = 128
S = 16
KC = 2
ITERS = 4
PB = 2
NB = 512
N = 65536
KB = 16
NBC = 64
N_COLS = 8


def plant(result, own_key, least, largest):
    shape = result.shape
    spot = [jax.random.randint(jax.random.fold_in(own_key, axis), (), 0, shape[axis]) for axis in range(len(shape))]
    result = result.at[tuple(spot)].set(least)
    longest = shape.index(max(shape))
    spot[longest] = (spot[longest] + 1) % shape[longest]
    return result.at[tuple(spot)].set(largest)


def level_of(stream_key, dims, shards, smallest, top_value):
    def one(dim, parts):
        draws = jax.random.uniform(jax.random.fold_in(jax.random.fold_in(stream_key, 6), dim), (parts,), jnp.float32, smallest / len(shards), top_value / len(shards))
        return jnp.repeat(jnp.exp(draws), dims[dim] // parts).reshape((-1,) + (1,) * (len(dims) - dim - 1))

    gain = one(*shards[0])
    for cut in shards[1:]:
        gain = gain * one(*cut)
    return gain


def noise(own_key, shape, scale, reach, shards=(), held_as=jnp.bfloat16):
    array = jax.random.normal(own_key, shape, jnp.float32) * scale
    if len(shards) > 0:
        array = level_of(own_key, shape, shards, -0.22, 0.18) * array
    return jnp.clip(array, min=-reach, max=reach).astype(held_as)


def setup_inputs(seed: int = 0) -> dict:
    seeds = jax.random.split(jax.random.key(seed), 6)
    return {
        "rhs": noise(seeds[0], (N, S), 1.0, 6.0, ((0, 256),), jnp.float32),
        "diagonal": jnp.clip(jnp.exp(math.log(16.0) - 2.7725887 * jax.random.uniform(seeds[1], (N,), jnp.float32) ** level_of(seeds[1], (N,), ((0, 256),), -0.2, 0.2)), 1.0, 16.0),
        "blocks": noise(seeds[2], (NB, KB, BS, BS), (3 * BS * KB) ** -0.5, 0.078125, ((0, 32), (1, 8)), jnp.float32),
        "block_cols": plant(jax.random.randint(seeds[3], (NB, KB), 0, NBC), jax.random.fold_in(seeds[3], 1), 0, NBC - 1).astype(jnp.int32),
        "counts": plant(jax.random.randint(seeds[4], (NB, N_COLS), 1, KC + 1), jax.random.fold_in(seeds[4], 1), 1, KC).astype(jnp.int32),
    }


def solve_block(matrix, right):
    size = matrix.shape[0]
    joined = jnp.concatenate([matrix, right], axis=1)
    for index in range(size):
        pivot_row = joined[index] / joined[index, index]
        joined = joined - joined[:, index:index + 1] * pivot_row[None, :]
        joined = joined.at[index].set(pivot_row)
    return joined[:, size:]


def gram(left, right):
    return jnp.dot(left.T, right, precision=lax.Precision.HIGHEST)


def times_block(vectors, small):
    return jnp.dot(vectors, small, precision=lax.Precision.HIGHEST)


def reference(rhs, diagonal, blocks, block_cols, counts):
    slot = jnp.arange(KB, dtype=jnp.int32)
    group = slot // KC
    within = slot % KC
    used = (within[None, :] < counts[:, group]).astype(jnp.float32)
    target = (block_cols // PB) * (N_COLS * PB) + group[None, :] * PB + block_cols % PB
    target = target.astype(jnp.int32)

    def apply(vectors):
        tiles = vectors.reshape(NB, BS, S)
        picked = tiles[target] * used[:, :, None, None]
        product = jnp.einsum("bkij,bkjs->bis", blocks, picked, precision=lax.Precision.HIGHEST)
        return diagonal[:, None] * vectors + product.reshape(N, S)

    solution = jnp.zeros_like(rhs)
    residual = rhs
    direction = rhs
    shadow = rhs
    for iteration in range(ITERS):
        image = apply(direction)
        matrix = gram(shadow, image)
        right = gram(shadow, residual)
        alpha = solve_block(matrix, right)
        middle = residual - times_block(image, alpha)
        second = apply(middle)
        omega = jnp.sum(second * middle) / jnp.sum(second * second)
        cross = gram(shadow, second)
        solution = solution + times_block(direction, alpha) + omega * middle
        residual = middle - omega * second
        beta = -solve_block(matrix, cross)
        direction = residual + times_block(direction - omega * image, beta)
    return solution
```

```python
import jax
import jax.numpy as jnp
from jax import lax
from jax.experimental import pallas as pl
from jax.experimental.pallas import tpu as pltpu
from jax.sharding import PartitionSpec as P

ITERS = 4
S = 16
BS = 128
F32 = jnp.float32
HI = lax.Precision.HIGHEST
VMEM = pl.BlockSpec(memory_space=pltpu.VMEM)
SMEM = pl.BlockSpec(memory_space=pltpu.SMEM)
TILE = 8


def sds(*shape, dtype=F32):
    return jax.ShapeDtypeStruct(shape, dtype)


def call(body, outs, specs, *args, name, scratch=()):
    return pl.pallas_call(
        body,
        out_shape=outs,
        in_specs=specs,
        out_specs=jax.tree.map(lambda _: VMEM, outs),
        scratch_shapes=scratch,
        name=name,
    )(*args)


def dot(a, b, contract=((1,), (0,))):
    return lax.dot_general(a, b, (contract, ((), ())), precision=HI, preferred_element_type=F32)


def bdot(a, b):
    return lax.dot_general(a, b, (((1,), (0,)), ((), ())), preferred_element_type=F32)


def halves(x):
    high = x.astype(jnp.bfloat16)
    return high, (x - high.astype(F32)).astype(jnp.bfloat16)


def wide(ref, at=()):
    return jnp.concatenate([ref[(*at, slice(0, S))], ref[(*at, slice(S, 2 * S))]], axis=1)


def spread(ref, value, tile):
    for k in range(ref.shape[0]):
        ref[k, 0:S] = value[:, :BS]
        ref[k, S : 2 * S] = value[:, BS:]
        ref[k, 2 * S : 2 * S + TILE] = tile


def solve(matrix, right):
    joined = jnp.concatenate([matrix, right], axis=1)
    row = lax.broadcasted_iota(jnp.int32, joined.shape, 0)
    for i in range(S):
        pivot = joined[i : i + 1, :] / joined[i : i + 1, i : i + 1]
        joined = jnp.where(row == i, pivot, joined - joined[:, i : i + 1] * pivot)
    return joined[:, S:]


def mix(vectors, small):
    return dot(small.T, vectors)


def grams(left, right):
    return dot(left, right, ((1,), (1,)))


def pack(products, extra=None):
    if extra is not None:
        row = lax.broadcasted_iota(jnp.int32, products.shape, 0)
        col = lax.broadcasted_iota(jnp.int32, products.shape, 1)
        for k, value in enumerate(extra):
            products = jnp.where((row == 0) & (col == S + k), value, products)
    return jnp.concatenate([products[8 * g : 8 * g + 8] for g in range(4)], axis=1)


def unpack(tile):
    whole = jnp.concatenate([tile[:, 32 * g : 32 * g + 32] for g in range(4)], axis=0)
    return whole[:S, :S], whole[:S, S:], whole[S:, :S], whole[S:, S:]


def total(ref):
    value = ref[0]
    for k in range(1, ref.shape[0]):
        value = value + ref[k]
    image = jnp.concatenate([value[0:S], value[S : 2 * S]], axis=1)
    return image, value[2 * S :]


def entire(x):
    return jnp.sum(jnp.sum(x, axis=1, keepdims=True), axis=0, keepdims=True)


def prepare_body(blocks, shadow_rows, cols, counts, core, packed, mine, other, acc):
    acc[...] = jnp.zeros_like(acc)

    def step(i, _):
        piece = shadow_rows[i // 2, pl.ds(pl.multiple_of((i % 2) * S, S), S), :]
        for k in range(2):
            keep = (k < counts[i, 0]).astype(F32)
            block = blocks[i, k] * keep
            target = cols[i, k]
            acc[target] += dot(piece, block)
            high, low = halves(block.T)
            packed[i, k * BS : (k + 1) * BS, 0:BS] = high
            packed[i, k * BS : (k + 1) * BS, BS : 2 * BS] = low
        return 0

    lax.fori_loop(0, 16, step, 0)
    me = core[0]
    for m in range(16):
        for b in range(2):
            mine[m, b * S : (b + 1) * S] = acc[m * 4 + me * 2 + b]
            other[m, b * S : (b + 1) * S] = acc[m * 4 + (1 - me) * 2 + b]


def product_body(own, peer, packed, cols, core, out):
    me = core[0]
    rows = own.shape[1]
    if rows > 2 * S:
        tile = own[0, 2 * S :]
        tile2 = peer[0, 2 * S :]
        for m in range(1, 16):
            tile = tile + own[m, 2 * S :]
            tile2 = tile2 + peer[m, 2 * S :]
        tile = tile + tile2
    for i in range(16):
        picked = []
        for k in range(2):
            col = cols[i, k]
            m = col // 4
            b = pl.multiple_of((col % 2) * S, S)
            here = own[m, pl.ds(b, S), :]
            there = peer[m, pl.ds(b, S), :]
            picked.append(jnp.where((col // 2) % 2 == me, here, there))
        high, low = halves(jnp.concatenate(picked, axis=1))
        result = bdot(jnp.concatenate([high, low], axis=0), packed[i])
        result = (result[:S, :BS] + result[:S, BS:]) + (result[S:, :BS] + result[S:, BS:])
        out[i // 2, (i % 2) * S : (i % 2 + 1) * S] = result
    if rows > 2 * S:
        for c in range(8):
            out[c, 2 * S :] = tile


def first_body(parts, arrived, shadow, diag, image, weights, message):
    value, _ = total(parts)
    rhs = shadow[...]
    v = value + diag[...] * rhs
    w = arrived[0, 0 : 2 * S]
    for m in range(1, 16):
        w = w + arrived[m, 0 : 2 * S]
    w = jnp.concatenate([w[0:S], w[S:]], axis=1) + diag[...] * rhs
    image[...] = v
    weights[...] = w
    products = grams(jnp.concatenate([w, rhs], axis=0), jnp.concatenate([v, rhs], axis=0))
    spread(message, v, pack(products))


def second_half(t, q, v, p, x, matrix, cross, w, s, u_out, base_out, t_out, cross_out, message):
    beta = -solve(matrix, cross)
    u = t + mix(v, beta)
    u_out[...] = u
    base_out[...] = q + mix(p, beta)
    t_out[...] = t
    cross_out[...] = cross
    products = grams(jnp.concatenate([w, s], axis=0), jnp.concatenate([u, q], axis=0))
    spread(message, u, pack(products, (entire(t * t), entire(t * q))))


def lead_body(parts, shadow, diag, image, weights, q_out, x_out, u_out, base_out, t_out, cross_out, message):
    value, tile = total(parts)
    s = shadow[...]
    v = image[...]
    z = value + diag[...] * v
    w_v, _, matrix, right = unpack(tile)
    alpha = solve(matrix, right)
    t = v - mix(z, alpha)
    q = s - mix(v, alpha)
    cross = matrix - dot(w_v, alpha)
    q_out[...] = q
    x_out[...] = mix(s, alpha)
    second_half(
        t, q, v, s, None, matrix, cross, weights[...], s, u_out, base_out, t_out, cross_out, message
    )


def even_body(
    parts, shadow, diag, weights, q, x, u, base, t, cross, q_out, x_out, v_out, p_out, matrix_out, message
):
    value, tile = total(parts)
    y = value + diag[...] * u[...]
    w_u, sums, s_u, s_q = unpack(tile)
    omega = sums[0:1, 1:2] / sums[0:1, 0:1]
    matrix = s_u - omega * w_u
    right = s_q - omega * cross[...]
    alpha = solve(matrix, right)
    v = u[...] - omega * y
    p = base[...] - omega * u[...]
    middle = (q[...] - omega * t[...]) - mix(v, alpha)
    x_out[...] = x[...] + omega * q[...] + mix(p, alpha)
    q_out[...] = middle
    v_out[...] = v
    p_out[...] = p
    matrix_out[...] = matrix
    products = grams(
        jnp.concatenate([weights[...], shadow[...]], axis=0),
        jnp.concatenate([middle, middle], axis=0),
    )
    spread(message, middle, pack(products))


def odd_body(
    parts, shadow, diag, weights, q, v, p, matrix, u_out, base_out, t_out, cross_out, message
):
    value, tile = total(parts)
    t = value + diag[...] * q[...]
    cross = unpack(tile)[0]
    second_half(
        t, q[...], v[...], p[...], None, matrix[...], cross, weights[...], shadow[...],
        u_out, base_out, t_out, cross_out, message,
    )


def last_body(parts, diag, q, sums):
    value, _ = total(parts)
    t = value + diag[...] * q[...]
    lane = lax.broadcasted_iota(jnp.int32, (1, BS), 1)
    sums[...] = jnp.where(lane == 0, entire(t * t), jnp.where(lane == 1, entire(t * q[...]), 0.0))


def end_body(sums, x, q, out):
    value = jnp.sum(sums[...], axis=0, keepdims=True)
    omega = value[0:1, 1:2] / value[0:1, 0:1]
    out[...] = x[...] + omega * q[...]


def per_device(rhs, diagonal, blocks, block_cols, counts):
    rows = lax.axis_size("rows")
    core_groups = [list(range(c, rows, 2)) for c in range(2)]
    partner = [(r, r ^ 1) for r in range(rows)]
    core = (lax.axis_index("rows") % 2).astype(jnp.int32).reshape(1)
    shadow = rhs.T
    diag = diagonal.reshape(1, 2 * BS)
    vec = sds(S, 2 * BS)
    small = sds(S, S)
    message = sds(16, 2 * S + TILE, BS)

    def among(x):
        return lax.all_to_all(x, "rows", 0, 0, tiled=True, axis_index_groups=core_groups)

    def across(x):
        return lax.all_to_all(x, "cols", 0, 0, tiled=True)

    def product(own):
        peer = lax.ppermute(own, "rows", partner)
        out = call(
            product_body, sds(8, own.shape[1], BS), [VMEM, VMEM, VMEM, SMEM, SMEM],
            own, peer, packed, block_cols, core, name="product",
        )
        return across(out)

    piece = jnp.concatenate([shadow[:, :BS], shadow[:, BS:]], axis=0)
    shadow_rows = across(jnp.broadcast_to(piece[None], (8, 2 * S, BS)))
    packed, mine, other = call(
        prepare_body,
        (sds(16, 2 * BS, 2 * BS, dtype=jnp.bfloat16), sds(16, 2 * S, BS), sds(16, 2 * S, BS)),
        [VMEM, VMEM, SMEM, SMEM, SMEM],
        blocks, shadow_rows, block_cols, counts, core,
        name="prepare", scratch=[pltpu.VMEM((64, S, BS), F32)],
    )
    mine = mine + lax.ppermute(other, "rows", partner)
    both = jnp.concatenate([mine, jnp.broadcast_to(piece[None], (16, 2 * S, BS))], axis=1)
    arrived = among(both)
    parts = product(arrived[:, 2 * S :])
    v, w, msg = call(
        first_body, (vec, vec, message), [VMEM] * 4, parts, arrived, shadow, diag, name="first"
    )
    parts = product(among(msg))
    q, x, u, base, t, cross, msg = call(
        lead_body, (vec, vec, vec, vec, vec, small, message), [VMEM] * 5,
        parts, shadow, diag, v, w, name="lead",
    )
    for iteration in range(1, ITERS):
        parts = product(among(msg))
        q, x, v, p, matrix, msg = call(
            even_body, (vec, vec, vec, vec, small, message), [VMEM] * 10,
            parts, shadow, diag, w, q, x, u, base, t, cross, name="even",
        )
        parts = product(among(msg))
        if iteration < ITERS - 1:
            u, base, t, cross, msg = call(
                odd_body, (vec, vec, vec, small, message), [VMEM] * 8,
                parts, shadow, diag, w, q, v, p, matrix, name="odd",
            )
    sums = call(last_body, sds(1, BS), [VMEM] * 3, parts, diag, q, name="last")
    everyone = rows * lax.axis_size("cols")
    sums = jnp.broadcast_to(sums[None], (everyone, 1, BS))
    sums = lax.all_to_all(sums, ("rows", "cols"), 0, 0, tiled=True)
    out = call(end_body, vec, [VMEM] * 3, sums.reshape(everyone, BS), x, q, name="end")
    return out.T


def solution(mesh):
    in_specs = (
        P(("rows", "cols"), None),
        P(("rows", "cols")),
        P("rows", "cols", None, None),
        P("rows", "cols"),
        P("rows", "cols"),
    )
    out_specs = P(("rows", "cols"), None)
    return jax.shard_map(
        per_device, mesh=mesh, in_specs=in_specs, out_specs=out_specs, check_vma=False
    )
```

```python
import jax
import jax.numpy as jnp
from jax import lax
from jax.experimental import pallas as pl
from jax.experimental.pallas import tpu as pltpu
from jax.sharding import PartitionSpec as P

ITERS = 4
S = 16
BS = 128
F32 = jnp.float32
HI = lax.Precision.HIGHEST
VMEM = pl.BlockSpec(memory_space=pltpu.VMEM)
SMEM = pl.BlockSpec(memory_space=pltpu.SMEM)
TILE = 8


def sds(*shape, dtype=F32):
    return pltpu.VMEM(shape, dtype)


def call(body, outs, specs, *args, name, scratch=()):
    args = [
        pltpu.with_memory_space_constraint(a, pltpu.VMEM) if spec is VMEM else a
        for a, spec in zip(args, specs)
    ]
    return pl.pallas_call(
        body,
        out_shape=outs,
        in_specs=specs,
        out_specs=tuple(VMEM for _ in outs) if isinstance(outs, tuple) else VMEM,
        scratch_shapes=scratch,
        name=name,
        compiler_params=pltpu.CompilerParams(vmem_limit_bytes=8 << 20),
    )(*args)


def dot(a, b, contract=((1,), (0,))):
    return lax.dot_general(a, b, (contract, ((), ())), precision=HI, preferred_element_type=F32)


def bdot(a, b):
    return lax.dot_general(a, b, (((1,), (0,)), ((), ())), preferred_element_type=F32)


def halves(x):
    high = x.astype(jnp.bfloat16)
    return high, (x - high.astype(F32)).astype(jnp.bfloat16)


def chip_of(seat):
    return (seat // 2 % 2) * 8 + (seat % 2) * 4 + seat // 4


def seat_of(chip):
    return (chip % 4) * 4 + (chip // 8) * 2 + chip // 4 % 2


def wide(ref, at=()):
    return jnp.concatenate([ref[(*at, slice(0, S))], ref[(*at, slice(S, 2 * S))]], axis=1)


def spread(ref, value, tile):
    for k in range(ref.shape[0]):
        ref[k, 0:S] = value[:, :BS]
        ref[k, S : 2 * S] = value[:, BS:]
        ref[k, 2 * S : 2 * S + TILE] = tile


def solve(matrix, right):
    joined = jnp.concatenate([matrix, right], axis=1)
    row = lax.broadcasted_iota(jnp.int32, joined.shape, 0)
    for i in range(S):
        pivot = joined[i : i + 1, :] / joined[i : i + 1, i : i + 1]
        joined = jnp.where(row == i, pivot, joined - joined[:, i : i + 1] * pivot)
    return joined[:, S:]


def mix(vectors, small):
    return dot(small.T, vectors)


def grams(left, right):
    return dot(left, right, ((1,), (1,)))


def pack(products, extra=None):
    if extra is not None:
        row = lax.broadcasted_iota(jnp.int32, products.shape, 0)
        col = lax.broadcasted_iota(jnp.int32, products.shape, 1)
        for k, value in enumerate(extra):
            products = jnp.where((row == 0) & (col == S + k), value, products)
    return jnp.concatenate([products[8 * g : 8 * g + 8] for g in range(4)], axis=1)


def unpack(tile):
    whole = jnp.concatenate([tile[:, 32 * g : 32 * g + 32] for g in range(4)], axis=0)
    return whole[:S, :S], whole[:S, S:], whole[S:, :S], whole[S:, S:]


def total(ref):
    value = ref[0]
    for k in range(1, ref.shape[0]):
        value = value + ref[k]
    image = jnp.concatenate([value[0:S], value[S : 2 * S]], axis=1)
    return image, value[2 * S :]


def entire(x):
    return jnp.sum(jnp.sum(x, axis=1, keepdims=True), axis=0, keepdims=True)


def prepare_body(blocks, shadow_rows, cols, counts, core, packed, mine, other, acc):
    acc[...] = jnp.zeros_like(acc)

    def step(i, _):
        piece = shadow_rows[i // 2, pl.ds(pl.multiple_of((i % 2) * S, S), S), :]
        for k in range(2):
            keep = (k < counts[i, 0]).astype(F32)
            block = blocks[i, k] * keep
            target = cols[i, k]
            acc[target] += dot(piece, block)
            high, low = halves(block.T)
            packed[i, k * BS : (k + 1) * BS, 0:BS] = high
            packed[i, k * BS : (k + 1) * BS, BS : 2 * BS] = low
        return 0

    lax.fori_loop(0, 16, step, 0)
    me = core[0]
    for m in range(16):
        for b in range(2):
            mine[m, b * S : (b + 1) * S] = acc[chip_of(m) * 4 + me * 2 + b]
            other[m, b * S : (b + 1) * S] = acc[chip_of(m) * 4 + (1 - me) * 2 + b]


def product_body(own, peer, packed, cols, core, out):
    me = core[0]
    rows = own.shape[1]
    if rows > 2 * S:
        tile = own[0, 2 * S :]
        tile2 = peer[0, 2 * S :]
        for m in range(1, 16):
            tile = tile + own[m, 2 * S :]
            tile2 = tile2 + peer[m, 2 * S :]
        tile = tile + tile2
    for i in range(16):
        picked = []
        for k in range(2):
            col = cols[i, k]
            m = seat_of(col // 4)
            b = pl.multiple_of((col % 2) * S, S)
            here = own[m, pl.ds(b, S), :]
            there = peer[m, pl.ds(b, S), :]
            picked.append(jnp.where((col // 2) % 2 == me, here, there))
        high, low = halves(jnp.concatenate(picked, axis=1))
        result = bdot(jnp.concatenate([high, low], axis=0), packed[i])
        result = (result[:S, :BS] + result[:S, BS:]) + (result[S:, :BS] + result[S:, BS:])
        out[i // 2, (i % 2) * S : (i % 2 + 1) * S] = result
    if rows > 2 * S:
        for c in range(8):
            out[c, 2 * S :] = tile


def first_body(parts, arrived, shadow, diag, image, weights, message):
    value, _ = total(parts)
    rhs = shadow[...]
    v = value + diag[...] * rhs
    w = arrived[0, 0 : 2 * S]
    for m in range(1, 16):
        w = w + arrived[m, 0 : 2 * S]
    w = jnp.concatenate([w[0:S], w[S:]], axis=1) + diag[...] * rhs
    image[...] = v
    weights[...] = w
    products = grams(jnp.concatenate([w, rhs], axis=0), jnp.concatenate([v, rhs], axis=0))
    spread(message, v, pack(products))


def second_half(t, q, v, p, x, matrix, cross, w, s, u_out, base_out, t_out, cross_out, message):
    beta = -solve(matrix, cross)
    u = t + mix(v, beta)
    u_out[...] = u
    base_out[...] = q + mix(p, beta)
    t_out[...] = t
    cross_out[...] = cross
    products = grams(jnp.concatenate([w, s], axis=0), jnp.concatenate([u, q], axis=0))
    spread(message, u, pack(products, (entire(t * t), entire(t * q))))


def lead_body(parts, shadow, diag, image, weights, q_out, x_out, u_out, base_out, t_out, cross_out, message):
    value, tile = total(parts)
    s = shadow[...]
    v = image[...]
    z = value + diag[...] * v
    w_v, _, matrix, right = unpack(tile)
    alpha = solve(matrix, right)
    t = v - mix(z, alpha)
    q = s - mix(v, alpha)
    cross = matrix - dot(w_v, alpha)
    q_out[...] = q
    x_out[...] = mix(s, alpha)
    second_half(
        t, q, v, s, None, matrix, cross, weights[...], s, u_out, base_out, t_out, cross_out, message
    )


def even_body(
    parts, shadow, diag, weights, q, x, u, base, t, cross, q_out, x_out, v_out, p_out, matrix_out, message
):
    value, tile = total(parts)
    y = value + diag[...] * u[...]
    w_u, sums, s_u, s_q = unpack(tile)
    omega = sums[0:1, 1:2] / sums[0:1, 0:1]
    matrix = s_u - omega * w_u
    right = s_q - omega * cross[...]
    alpha = solve(matrix, right)
    v = u[...] - omega * y
    p = base[...] - omega * u[...]
    middle = (q[...] - omega * t[...]) - mix(v, alpha)
    x_out[...] = x[...] + omega * q[...] + mix(p, alpha)
    q_out[...] = middle
    v_out[...] = v
    p_out[...] = p
    matrix_out[...] = matrix
    products = grams(
        jnp.concatenate([weights[...], shadow[...]], axis=0),
        jnp.concatenate([middle, middle], axis=0),
    )
    spread(message, middle, pack(products))


def odd_body(
    parts, shadow, diag, weights, q, v, p, matrix, u_out, base_out, t_out, cross_out, message
):
    value, tile = total(parts)
    t = value + diag[...] * q[...]
    cross = unpack(tile)[0]
    second_half(
        t, q[...], v[...], p[...], None, matrix[...], cross, weights[...], shadow[...],
        u_out, base_out, t_out, cross_out, message,
    )


def last_body(parts, diag, q, sums):
    value, _ = total(parts)
    t = value + diag[...] * q[...]
    lane = lax.broadcasted_iota(jnp.int32, (1, BS), 1)
    sums[...] = jnp.where(lane == 0, entire(t * t), jnp.where(lane == 1, entire(t * q[...]), 0.0))


def end_body(sums, x, q, out):
    value = jnp.sum(sums[...], axis=0, keepdims=True)
    omega = value[0:1, 1:2] / value[0:1, 0:1]
    out[...] = x[...] + omega * q[...]


def per_device(rhs, diagonal, blocks, block_cols, counts):
    rows = lax.axis_size("rows")
    core_groups = [[2 * chip_of(m) + c for m in range(rows // 2)] for c in range(2)]
    partner = [(r, r ^ 1) for r in range(rows)]
    core = (lax.axis_index("rows") % 2).astype(jnp.int32).reshape(1)
    shadow = rhs.T
    diag = diagonal.reshape(1, 2 * BS)
    vec = sds(S, 2 * BS)
    small = sds(S, S)
    message = sds(16, 2 * S + TILE, BS)

    def among(x):
        return lax.all_to_all(x, "rows", 0, 0, tiled=True, axis_index_groups=core_groups)

    def across(x):
        return lax.all_to_all(x, "cols", 0, 0, tiled=True)

    def product(own):
        peer = lax.ppermute(own, "rows", partner)
        out = call(
            product_body, sds(8, own.shape[1], BS), [VMEM, VMEM, VMEM, SMEM, SMEM],
            own, peer, packed, block_cols, core, name="product",
        )
        return across(out)

    piece = jnp.concatenate([shadow[:, :BS], shadow[:, BS:]], axis=0)
    shadow_rows = across(jnp.broadcast_to(piece[None], (8, 2 * S, BS)))
    packed, mine, other = call(
        prepare_body,
        (sds(16, 2 * BS, 2 * BS, dtype=jnp.bfloat16), sds(16, 2 * S, BS), sds(16, 2 * S, BS)),
        [VMEM, VMEM, SMEM, SMEM, SMEM],
        blocks, shadow_rows, block_cols, counts, core,
        name="prepare", scratch=[pltpu.VMEM((64, S, BS), F32)],
    )
    mine = mine + lax.ppermute(other, "rows", partner)
    both = jnp.concatenate([mine, jnp.broadcast_to(piece[None], (16, 2 * S, BS))], axis=1)
    arrived = among(both)
    parts = product(arrived[:, 2 * S :])
    v, w, msg = call(
        first_body, (vec, vec, message), [VMEM] * 4, parts, arrived, shadow, diag, name="first"
    )
    parts = product(among(msg))
    q, x, u, base, t, cross, msg = call(
        lead_body, (vec, vec, vec, vec, vec, small, message), [VMEM] * 5,
        parts, shadow, diag, v, w, name="lead",
    )
    for iteration in range(1, ITERS):
        parts = product(among(msg))
        q, x, v, p, matrix, msg = call(
            even_body, (vec, vec, vec, vec, small, message), [VMEM] * 10,
            parts, shadow, diag, w, q, x, u, base, t, cross, name="even",
        )
        parts = product(among(msg))
        if iteration < ITERS - 1:
            u, base, t, cross, msg = call(
                odd_body, (vec, vec, vec, small, message), [VMEM] * 8,
                parts, shadow, diag, w, q, v, p, matrix, name="odd",
            )
    sums = call(last_body, sds(1, BS), [VMEM] * 3, parts, diag, q, name="last")
    everyone = rows * lax.axis_size("cols")
    sums = jnp.broadcast_to(sums[None], (everyone, 1, BS))
    sums = lax.all_to_all(sums, ("rows", "cols"), 0, 0, tiled=True)
    out = call(end_body, vec, [VMEM] * 3, sums.reshape(everyone, BS), x, q, name="end")
    return out.T


def solution(mesh):
    in_specs = (
        P(("rows", "cols"), None),
        P(("rows", "cols")),
        P("rows", "cols", None, None),
        P("rows", "cols"),
        P("rows", "cols"),
    )
    out_specs = P(("rows", "cols"), None)
    return jax.shard_map(
        per_device, mesh=mesh, in_specs=in_specs, out_specs=out_specs, check_vma=False
    )
```

```python
import jax
import jax.numpy as jnp
from jax import lax
from jax.experimental import pallas as pl
from jax.experimental.pallas import tpu as pltpu
from jax.sharding import PartitionSpec as P

ITERS = 4
S = 16
BS = 128
F32 = jnp.float32
HI = lax.Precision.HIGHEST
VMEM = pl.BlockSpec(memory_space=pltpu.VMEM)
SMEM = pl.BlockSpec(memory_space=pltpu.SMEM)
HBM = pl.BlockSpec(memory_space=pltpu.HBM)
TILE = 8


def sds(*shape, dtype=F32):
    return pltpu.VMEM(shape, dtype)


def call(body, outs, specs, *args, name, scratch=()):
    args = [
        a if spec is SMEM else pltpu.with_memory_space_constraint(a, spec.memory_space)
        for a, spec in zip(args, specs)
    ]
    return pl.pallas_call(
        body,
        out_shape=outs,
        in_specs=specs,
        out_specs=tuple(VMEM for _ in outs) if isinstance(outs, tuple) else VMEM,
        scratch_shapes=scratch,
        name=name,
        compiler_params=pltpu.CompilerParams(vmem_limit_bytes=8 << 20),
    )(*args)


def dot(a, b, contract=((1,), (0,))):
    return lax.dot_general(a, b, (contract, ((), ())), precision=HI, preferred_element_type=F32)


def bdot(a, b):
    return lax.dot_general(a, b, (((1,), (0,)), ((), ())), preferred_element_type=F32)


def halves(x):
    high = x.astype(jnp.bfloat16)
    return high, (x - high.astype(F32)).astype(jnp.bfloat16)


def wide(ref, at=()):
    return jnp.concatenate([ref[(*at, slice(0, S))], ref[(*at, slice(S, 2 * S))]], axis=1)


def spread(ref, value, tile):
    for k in range(ref.shape[0]):
        ref[k, 0:S] = value[:, :BS]
        ref[k, S : 2 * S] = value[:, BS:]
        ref[k, 2 * S : 2 * S + TILE] = tile


def narrow(x):
    return jnp.concatenate([x[:, :BS], x[:, BS:]], axis=0)


def solve(matrix, right):
    joined = jnp.concatenate([matrix, right], axis=1)
    row = lax.broadcasted_iota(jnp.int32, joined.shape, 0)
    for i in range(S):
        column = jnp.broadcast_to(joined[:, i : i + 1], joined.shape)
        pivot = joined[i : i + 1, :] / column[i : i + 1, :]
        joined = jnp.where(row == i, pivot, joined - column * pivot)
    return joined[:, S:]


def mix(vectors, small):
    return dot(small.T, vectors)


def grams(left, right):
    return dot(left, right, ((1,), (1,)))


def pack(products, extra=None):
    if extra is not None:
        row = lax.broadcasted_iota(jnp.int32, products.shape, 0)
        col = lax.broadcasted_iota(jnp.int32, products.shape, 1)
        for k, value in enumerate(extra):
            products = jnp.where((row == 0) & (col == S + k), value, products)
    return jnp.concatenate([products[8 * g : 8 * g + 8] for g in range(4)], axis=1)


def unpack(tile):
    whole = jnp.concatenate([tile[:, 32 * g : 32 * g + 32] for g in range(4)], axis=0)
    return whole[:S, :S], whole[:S, S:], whole[S:, :S], whole[S:, S:]


def total(ref, first=0, last=None):
    value = ref[0, first:last]
    for k in range(1, ref.shape[0]):
        value = value + ref[k, first:last]
    image = jnp.concatenate([value[0:S], value[S : 2 * S]], axis=1)
    return image, value[2 * S :]


def entire(x):
    return jnp.sum(jnp.sum(x, axis=1, keepdims=True), axis=0, keepdims=True)


def fetch(blocks, held, done):
    copies = [pltpu.make_async_copy(blocks.at[i], held.at[i], done.at[i]) for i in range(16)]
    for copy in copies:
        copy.start()
    return copies


def prepare_body(source, counts, packed, blocks, done):
    copies = fetch(source, blocks, done)
    for i in range(16):
        copies[i].wait()
        for k in range(2):
            keep = (k < counts[0, i]).astype(F32)
            high, low = halves((blocks[i, k] * keep).T)
            packed[i, k * BS : (k + 1) * BS, 0:BS] = high
            packed[i, k * BS : (k + 1) * BS, BS : 2 * BS] = low


def transposed_body(source, arrived, cols, counts, core, mine, other, acc, blocks, done):
    copies = fetch(source, blocks, done)
    acc[...] = jnp.zeros_like(acc)
    for i in range(16):
        copies[i].wait()
        b = 2 * S + i % 2 * S
        piece = arrived[i // 2, b : b + S]
        for k in range(2):
            keep = (k < counts[0, i]).astype(F32)
            acc[cols[k, i]] += dot(piece * keep, blocks[i, k])
    me = core[0]
    for m in range(16):
        for b in range(2):
            mine[m, b * S : (b + 1) * S] = acc[m * 4 + me * 2 + b]
            other[m, b * S : (b + 1) * S] = acc[m * 4 + (1 - me) * 2 + b]


def product_body(own, peer, packed, cols, core, *rest):
    piece, out = rest if len(rest) == 2 else (None, *rest)
    me = core[0]
    if piece is None:
        extra = own[0, 2 * S : 2 * S + TILE]
        extra2 = peer[0, 2 * S : 2 * S + TILE]
        for m in range(1, 16):
            extra = extra + own[m, 2 * S : 2 * S + TILE]
            extra2 = extra2 + peer[m, 2 * S : 2 * S + TILE]
        extra = extra + extra2
    else:
        extra = piece[...]
    for i in range(16):
        picked = []
        for k in range(2):
            col = cols[k, i]
            m = col // 4
            b = pl.multiple_of((col % 2) * S, S)
            here = own[m, pl.ds(b, S), :]
            there = peer[m, pl.ds(b, S), :]
            picked.append(jnp.where((col // 2) % 2 == me, here, there))
        high, low = halves(jnp.concatenate(picked, axis=1))
        result = bdot(jnp.concatenate([high, low], axis=0), packed[i])
        result = (result[:S, :BS] + result[:S, BS:]) + (result[S:, :BS] + result[S:, BS:])
        out[i // 2, (i % 2) * S : (i % 2 + 1) * S] = result
    for c in range(8):
        out[c, 2 * S :] = extra


def first_body(parts, mine, theirs, shadow, diag, image, message):
    value, _ = total(parts, 0, 2 * S)
    s = shadow[...]
    v = value + diag[...] * s
    image[...] = v
    products = grams(jnp.concatenate([s, s], axis=0), jnp.concatenate([v, s], axis=0))
    spread(message, v, pack(products))
    for m in range(16):
        message[m, 2 * S + TILE :] = mine[m] + theirs[m]


def lead_body(
    parts, arrived, shadow, diag, image,
    z_out, t_out, q_out, x_out, weights, matrix_out, right_out, message,
):
    value, tile = total(parts)
    s = shadow[...]
    v = image[...]
    z = value + diag[...] * v
    _, _, matrix, right = unpack(tile)
    alpha = solve(matrix, right)
    t = v - mix(z, alpha)
    q = s - mix(v, alpha)
    w = total(arrived, 2 * S + TILE)[0] + diag[...] * s
    z_out[...] = z
    t_out[...] = t
    q_out[...] = q
    x_out[...] = mix(s, alpha)
    weights[...] = w
    matrix_out[...] = matrix
    right_out[...] = right - dot(matrix, alpha)
    products = grams(jnp.concatenate([s, w], axis=0), jnp.concatenate([t, v], axis=0))
    spread(message, t, pack(products, (entire(t * t), entire(t * q))))


def middle_step(
    y, u, base, t, q, x, w, s, w_u, s_u, s_q, cross, tt, tq, q_out, x_out, v_out, p_out, matrix_out, message
):
    omega = tq / tt
    matrix = s_u - omega * w_u
    right = s_q - omega * cross
    alpha = solve(matrix, right)
    v = u - omega * y
    p = base - omega * u
    middle = (q - omega * t) - mix(v, alpha)
    x_out[...] = x + omega * q + mix(p, alpha)
    q_out[...] = middle
    v_out[...] = v
    p_out[...] = p
    matrix_out[...] = matrix
    products = grams(jnp.concatenate([w, s], axis=0), jnp.concatenate([middle, middle], axis=0))
    spread(message, middle, pack(products))


def second_body(
    parts, shadow, diag, image, weights, z, t, q, x, matrix, right, *outs
):
    value, tile = total(parts)
    f = value + diag[...] * t[...]
    cross, sums, w_t, w_v = unpack(tile)
    beta = -solve(matrix[...], cross)
    u = t[...] + mix(image[...], beta)
    y = f + mix(z[...], beta)
    base = q[...] + mix(shadow[...], beta)
    middle_step(
        y, u, base, t[...], q[...], x[...], weights[...], shadow[...],
        w_t + dot(w_v, beta), cross + dot(matrix[...], beta), right[...], cross,
        sums[0:1, 0:1], sums[0:1, 1:2], *outs,
    )


def even_body(parts, shadow, diag, weights, q, x, u, base, t, cross, *outs):
    value, tile = total(parts)
    y = value + diag[...] * u[...]
    w_u, sums, s_u, s_q = unpack(tile)
    middle_step(
        y, u[...], base[...], t[...], q[...], x[...], weights[...], shadow[...],
        w_u, s_u, s_q, cross[...], sums[0:1, 0:1], sums[0:1, 1:2], *outs,
    )


def odd_body(
    parts, shadow, diag, weights, q, v, p, matrix, u_out, base_out, t_out, cross_out, message
):
    value, tile = total(parts)
    t = value + diag[...] * q[...]
    cross = unpack(tile)[0]
    beta = -solve(matrix[...], cross)
    u = t + mix(v[...], beta)
    u_out[...] = u
    base_out[...] = q[...] + mix(p[...], beta)
    t_out[...] = t
    cross_out[...] = cross
    products = grams(
        jnp.concatenate([weights[...], shadow[...]], axis=0), jnp.concatenate([u, q[...]], axis=0)
    )
    spread(message, u, pack(products, (entire(t * t), entire(t * q[...]))))


def last_body(parts, diag, q, sums):
    value, _ = total(parts)
    t = value + diag[...] * q[...]
    lane = lax.broadcasted_iota(jnp.int32, (1, BS), 1)
    sums[...] = jnp.where(lane == 0, entire(t * t), jnp.where(lane == 1, entire(t * q[...]), 0.0))


def end_body(sums, x, q, out):
    value = jnp.sum(sums[...], axis=0, keepdims=True)
    omega = value[0:1, 1:2] / value[0:1, 0:1]
    out[...] = x[...] + omega * q[...]


def per_device(rhs, diagonal, blocks, block_cols, counts):
    core = lax.axis_index("core").astype(jnp.int32).reshape(1)
    block_cols = block_cols.T
    counts = counts.T
    shadow = rhs.T
    diag = diagonal.reshape(1, 2 * BS)
    vec = sds(S, 2 * BS)
    small = sds(S, S)
    message = sds(16, 2 * S + TILE, BS)

    def among(x):
        return lax.all_to_all(x, ("x", "z"), 0, 0, tiled=True)

    def across(x):
        return lax.all_to_all(x, "cols", 0, 0, tiled=True)

    def product(own, *piece):
        peer = lax.ppermute(own, "core", [(0, 1), (1, 0)])
        out = call(
            product_body, sds(8, 2 * S + (2 * S if piece else TILE), BS),
            [VMEM, VMEM, VMEM, SMEM, SMEM] + [VMEM] * len(piece),
            own, peer, packed, block_cols, core, *piece, name="product",
        )
        return across(out)

    held = [pltpu.VMEM((16, 2, BS, BS), F32), pltpu.SemaphoreType.DMA((16,))]
    piece = jnp.concatenate([shadow[:, :BS], shadow[:, BS:]], axis=0)
    packed = call(
        prepare_body, sds(16, 2 * BS, 2 * BS, dtype=jnp.bfloat16), [HBM, SMEM],
        blocks, counts, name="prepare", scratch=held,
    )
    parts = product(among(jnp.broadcast_to(piece[None], (16, 2 * S, BS))), piece)
    mine, other = call(
        transposed_body, (sds(16, 2 * S, BS), sds(16, 2 * S, BS)), [HBM, VMEM, SMEM, SMEM, SMEM],
        blocks, parts, block_cols, counts, core,
        name="transposed", scratch=[pltpu.VMEM((64, S, BS), F32), *held],
    )
    theirs = lax.ppermute(other, "core", [(0, 1), (1, 0)])
    v, msg = call(
        first_body, (vec, sds(16, 4 * S + TILE, BS)), [VMEM] * 5,
        parts, mine, theirs, shadow, diag, name="first",
    )
    arrived = among(msg)
    z, t, q, x, w, matrix, right, msg = call(
        lead_body, (vec, vec, vec, vec, vec, small, small, message), [VMEM] * 5,
        product(arrived), arrived, shadow, diag, v, name="lead",
    )
    for iteration in range(1, ITERS):
        parts = product(among(msg))
        outs = (vec, vec, vec, vec, small, message)
        if iteration == 1:
            q, x, v, p, matrix, msg = call(
                second_body, outs, [VMEM] * 11,
                parts, shadow, diag, v, w, z, t, q, x, matrix, right, name="second",
            )
        else:
            q, x, v, p, matrix, msg = call(
                even_body, outs, [VMEM] * 10,
                parts, shadow, diag, w, q, x, u, base, t, cross, name="even",
            )
        parts = product(among(msg))
        if iteration < ITERS - 1:
            u, base, t, cross, msg = call(
                odd_body, (vec, vec, vec, small, message), [VMEM] * 8,
                parts, shadow, diag, w, q, v, p, matrix, name="odd",
            )
    sums = call(last_body, sds(1, BS), [VMEM] * 3, parts, diag, q, name="last")
    everyone = 2 * 16 * 8
    sums = jnp.broadcast_to(sums[None], (everyone, 1, BS))
    sums = lax.all_to_all(sums, ("x", "z", "core", "cols"), 0, 0, tiled=True)
    out = call(end_body, vec, [VMEM] * 3, sums.reshape(everyone, BS), x, q, name="end")
    return out.T


def solution(mesh):
    parts = ("x", "z", "core")
    mesh = jax.sharding.Mesh(mesh.devices.reshape(2, 8, 2, 8), (*parts, "cols"))
    in_specs = (
        P((*parts, "cols"), None),
        P((*parts, "cols")),
        P(parts, "cols", None, None),
        P(parts, "cols"),
        P(parts, "cols"),
    )
    out_specs = P((*parts, "cols"), None)
    return jax.shard_map(
        per_device, mesh=mesh, in_specs=in_specs, out_specs=out_specs, check_vma=False
    )
```

```python
import jax
import jax.numpy as jnp
from jax import lax
from jax.experimental import pallas as pl
from jax.experimental.pallas import tpu as pltpu
from jax.sharding import PartitionSpec as P

ITERS = 4
S = 16
BS = 128
F32 = jnp.float32
HI = lax.Precision.HIGHEST
VMEM = pl.BlockSpec(memory_space=pltpu.VMEM)
SMEM = pl.BlockSpec(memory_space=pltpu.SMEM)
HBM = pl.BlockSpec(memory_space=pltpu.HBM)
TILE = 8


def sds(*shape, dtype=F32):
    return pltpu.VMEM(shape, dtype)


def call(body, outs, specs, *args, name, scratch=()):
    args = [
        a if spec is SMEM else pltpu.with_memory_space_constraint(a, spec.memory_space)
        for a, spec in zip(args, specs)
    ]
    return pl.pallas_call(
        body,
        out_shape=outs,
        in_specs=specs,
        out_specs=tuple(VMEM for _ in outs) if isinstance(outs, tuple) else VMEM,
        scratch_shapes=scratch,
        name=name,
        compiler_params=pltpu.CompilerParams(vmem_limit_bytes=8 << 20),
    )(*args)


def dot(a, b, contract=((1,), (0,))):
    return lax.dot_general(a, b, (contract, ((), ())), precision=HI, preferred_element_type=F32)


def bdot(a, b):
    return lax.dot_general(a, b, (((1,), (0,)), ((), ())), preferred_element_type=F32)


def halves(x):
    high = x.astype(jnp.bfloat16)
    return high, (x - high.astype(F32)).astype(jnp.bfloat16)


def wide(ref, at=()):
    return jnp.concatenate([ref[(*at, slice(0, S))], ref[(*at, slice(S, 2 * S))]], axis=1)


def spread(ref, value, tile):
    for k in range(ref.shape[0]):
        ref[k, 0:S] = value[:, :BS]
        ref[k, S : 2 * S] = value[:, BS:]
        ref[k, 2 * S : 2 * S + TILE] = tile


def solve(matrix, right):
    joined = jnp.concatenate([matrix, right], axis=1)
    row = lax.broadcasted_iota(jnp.int32, joined.shape, 0)
    for i in range(S):
        column = jnp.broadcast_to(joined[:, i : i + 1], joined.shape)
        pivot = joined[i : i + 1, :] / column[i : i + 1, :]
        joined = jnp.where(row == i, pivot, joined - column * pivot)
    return joined[:, S:]


def mix(vectors, small):
    return dot(small.T, vectors)


def grams(left, right):
    return dot(left, right, ((1,), (1,)))


def pack(products, sums=()):
    lane = lax.broadcasted_iota(jnp.int32, (TILE, 2 * S), 1)
    row = lax.broadcasted_iota(jnp.int32, (TILE, 2 * S), 0)
    rest = jnp.zeros((TILE, 2 * S), F32)
    for k, value in enumerate(sums):
        rest = jnp.where((row == 0) & (lane == k), value, rest)
    return jnp.concatenate([products[:TILE], products[TILE:], rest, rest], axis=1)


def unpack(tile):
    whole = jnp.concatenate([tile[:, : 2 * S], tile[:, 2 * S : 4 * S]], axis=0)
    return whole[:, :S], whole[:, S:], tile[:, 4 * S :]


def total(ref, first=0, last=None):
    value = ref[0, first:last]
    for k in range(1, ref.shape[0]):
        value = value + ref[k, first:last]
    image = jnp.concatenate([value[0:S], value[S : 2 * S]], axis=1)
    return image, value[2 * S :]


def entire(x):
    return jnp.sum(jnp.sum(x, axis=1, keepdims=True), axis=0, keepdims=True)


def fetch(blocks, held, done):
    copies = [pltpu.make_async_copy(blocks.at[i], held.at[i], done.at[i]) for i in range(16)]
    for copy in copies:
        copy.start()
    return copies


def prepare_body(source, counts, packed, blocks, done):
    copies = fetch(source, blocks, done)
    for i in range(16):
        copies[i].wait()
        for k in range(2):
            keep = (k < counts[0, i]).astype(F32)
            high, low = halves((blocks[i, k] * keep).T)
            packed[i, k * BS : (k + 1) * BS, 0:BS] = high
            packed[i, k * BS : (k + 1) * BS, BS : 2 * BS] = low


def product_body(own, peer, packed, cols, core, out):
    me = core[0]
    for i in range(16):
        picked = []
        for k in range(2):
            col = cols[k, i]
            m = col // 4
            b = pl.multiple_of((col % 2) * S, S)
            here = own[m, pl.ds(b, S), :]
            there = peer[m, pl.ds(b, S), :]
            picked.append(jnp.where((col // 2) % 2 == me, here, there))
        high, low = halves(jnp.concatenate(picked, axis=1))
        result = bdot(jnp.concatenate([high, low], axis=0), packed[i])
        result = (result[:S, :BS] + result[:S, BS:]) + (result[S:, :BS] + result[S:, BS:])
        out[i // 2, (i % 2) * S : (i % 2 + 1) * S] = result
    if own.shape[1] > 2 * S:
        tile, tile2 = own[0, 2 * S :], peer[0, 2 * S :]
        for m in range(1, 16):
            tile = tile + own[m, 2 * S :]
            tile2 = tile2 + peer[m, 2 * S :]
        for c in range(8):
            out[c, 2 * S :] = tile + tile2


def first_body(parts, shadow, diag, image, message):
    value, _ = total(parts)
    s = shadow[...]
    v = value + diag[...] * s
    image[...] = v
    spread(message, v, pack(grams(s, jnp.concatenate([v, s], axis=0))))


def lead_step(parts, diag, image, forward, residual, direction, solution):
    value, tile = total(parts)
    v = image[...]
    z = value + diag[...] * v
    matrix, right, _ = unpack(tile)
    alpha = solve(matrix, right)
    q = residual[...] - mix(v, alpha)
    t = forward[...] - mix(z, alpha)
    x = mix(direction[...], alpha)
    if solution is not None:
        x = x + solution[...]
    return matrix, z, q, t, x


def lead_body(
    parts, shadow, diag, image, forward, residual, direction, *rest
):
    solution, (z_out, q_out, t_out, x_out, matrix_out, message) = rest[:-6], rest[-6:]
    matrix, z, q, t, x = lead_step(
        parts, diag, image, forward, residual, direction, solution[0] if solution else None
    )
    z_out[...] = z
    q_out[...] = q
    t_out[...] = t
    x_out[...] = x
    matrix_out[...] = matrix
    products = grams(shadow[...], jnp.concatenate([t, t], axis=0))
    spread(message, t, pack(products, (entire(t * t), entire(t * q))))


def follow_body(
    parts, shadow, diag, image, direction, z, q, t, x, matrix,
    v_out, f_out, r_out, p_out, x_out, message,
):
    value, tile = total(parts)
    middle = t[...]
    f = value + diag[...] * middle
    cross, _, sums = unpack(tile)
    omega = sums[0:1, 1:2] / sums[0:1, 0:1]
    beta = -solve(matrix[...], cross)
    v = image[...]
    u = middle + mix(v, beta)
    y = f + mix(z[...], beta)
    residual = q[...] - omega * middle
    image_new = u - omega * y
    v_out[...] = image_new
    f_out[...] = middle - omega * f
    r_out[...] = residual
    p_out[...] = residual + mix(direction[...] - omega * v, beta)
    x_out[...] = x[...] + omega * q[...]
    products = grams(shadow[...], jnp.concatenate([image_new, residual], axis=0))
    spread(message, image_new, pack(products))


def last_body(parts, diag, image, forward, residual, direction, solution, q_out, x_out, sums):
    _, _, q, t, x = lead_step(parts, diag, image, forward, residual, direction, solution)
    q_out[...] = q
    x_out[...] = x
    lane = lax.broadcasted_iota(jnp.int32, (1, BS), 1)
    sums[...] = jnp.where(lane == 0, entire(t * t), jnp.where(lane == 1, entire(t * q), 0.0))


def end_body(sums, x, q, out):
    value = jnp.sum(sums[...], axis=0, keepdims=True)
    omega = value[0:1, 1:2] / value[0:1, 0:1]
    out[...] = x[...] + omega * q[...]


def per_device(rhs, diagonal, blocks, block_cols, counts):
    core = lax.axis_index("core").astype(jnp.int32).reshape(1)
    block_cols = block_cols.T
    counts = counts.T
    shadow = rhs.T
    diag = diagonal.reshape(1, 2 * BS)
    vec = sds(S, 2 * BS)
    small = sds(S, S)
    message = sds(16, 2 * S + TILE, BS)

    def among(x):
        return lax.all_to_all(x, ("x", "z"), 0, 0, tiled=True)

    def across(x):
        return lax.all_to_all(x, "cols", 0, 0, tiled=True)

    def product(own):
        peer = lax.ppermute(own, "core", [(0, 1), (1, 0)])
        out = call(
            product_body, sds(8, own.shape[1], BS), [VMEM, VMEM, VMEM, SMEM, SMEM],
            own, peer, packed, block_cols, core, name="product",
        )
        return across(out)

    held = [pltpu.VMEM((16, 2, BS, BS), F32), pltpu.SemaphoreType.DMA((16,))]
    piece = jnp.concatenate([shadow[:, :BS], shadow[:, BS:]], axis=0)
    packed = call(
        prepare_body, sds(16, 2 * BS, 2 * BS, dtype=jnp.bfloat16), [HBM, SMEM],
        blocks, counts, name="prepare", scratch=held,
    )
    parts = product(among(jnp.broadcast_to(piece[None], (16, 2 * S, BS))))
    v, msg = call(first_body, (vec, message), [VMEM] * 3, parts, shadow, diag, name="first")
    f, r, p, x = v, shadow, shadow, ()
    for iteration in range(ITERS):
        parts = product(among(msg))
        if iteration == ITERS - 1:
            break
        z, q, t, x, matrix, msg = call(
            lead_body, (vec, vec, vec, vec, small, message), [VMEM] * (7 + len(x)),
            parts, shadow, diag, v, f, r, p, *x, name="lead",
        )
        parts = product(among(msg))
        v, f, r, p, x, msg = call(
            follow_body, (vec, vec, vec, vec, vec, message), [VMEM] * 10,
            parts, shadow, diag, v, p, z, q, t, x, matrix, name="follow",
        )
        x = (x,)
    q, x, sums = call(
        last_body, (vec, vec, sds(1, BS)), [VMEM] * 7,
        parts, diag, v, f, r, p, *x, name="last",
    )
    everyone = 2 * 16 * 8
    sums = jnp.broadcast_to(sums[None], (everyone, 1, BS))
    sums = lax.all_to_all(sums, ("x", "z", "core", "cols"), 0, 0, tiled=True)
    out = call(end_body, vec, [VMEM] * 3, sums.reshape(everyone, BS), x, q, name="end")
    return out.T


def solution(mesh):
    parts = ("x", "z", "core")
    mesh = jax.sharding.Mesh(mesh.devices.reshape(2, 8, 2, 8), (*parts, "cols"))
    in_specs = (
        P((*parts, "cols"), None),
        P((*parts, "cols")),
        P(parts, "cols", None, None),
        P(parts, "cols"),
        P(parts, "cols"),
    )
    out_specs = P((*parts, "cols"), None)
    return jax.shard_map(
        per_device, mesh=mesh, in_specs=in_specs, out_specs=out_specs, check_vma=False
    )
```

```python
import jax
import jax.numpy as jnp
from jax import lax
from jax.experimental import pallas as pl
from jax.experimental.pallas import tpu as pltpu
from jax.sharding import PartitionSpec as P


ITERS = 4
S = 16
BS = 128
F32 = jnp.float32
HI = lax.Precision.HIGHEST
VMEM = pl.BlockSpec(memory_space=pltpu.VMEM)
SMEM = pl.BlockSpec(memory_space=pltpu.SMEM)
HBM = pl.BlockSpec(memory_space=pltpu.HBM)
TILE = 8


def sds(*shape, dtype=F32):
    return pltpu.VMEM(shape, dtype)


def call(body, outs, specs, *args, scratch=()):
    args = [
        a if spec is SMEM else pltpu.with_memory_space_constraint(a, spec.memory_space)
        for a, spec in zip(args, specs)
    ]
    return pl.pallas_call(
        body,
        out_shape=outs,
        in_specs=specs,
        out_specs=tuple(VMEM for _ in outs) if isinstance(outs, tuple) else VMEM,
        scratch_shapes=scratch,
        compiler_params=pltpu.CompilerParams(vmem_limit_bytes=8 << 20),
    )(*args)


def dot(a, b, contract=((1,), (0,))):
    return lax.dot_general(a, b, (contract, ((), ())), precision=HI, preferred_element_type=F32)


def bdot(a, b):
    return lax.dot_general(a, b, (((1,), (0,)), ((), ())), preferred_element_type=F32)


def halves(x):
    high = x.astype(jnp.bfloat16)
    return high, (x - high.astype(F32)).astype(jnp.bfloat16)


def spread(ref, value, tile):
    for k in range(ref.shape[0]):
        ref[k, 0:S] = value[:, :BS]
        ref[k, S : 2 * S] = value[:, BS:]
        ref[k, 2 * S : 2 * S + TILE] = tile


def solve(matrix, right):
    joined = jnp.concatenate([matrix, right], axis=1)
    row = lax.broadcasted_iota(jnp.int32, joined.shape, 0)
    for i in range(S):
        column = jnp.broadcast_to(joined[:, i : i + 1], joined.shape)
        pivot = joined[i : i + 1, :] / column[i : i + 1, :]
        joined = jnp.where(row == i, pivot, joined - column * pivot)
    return joined[:, S:]


def mix(vectors, small):
    return dot(small.T, vectors)


def grams(left, right):
    return dot(left, right, ((1,), (1,)))


def pack(products, sums=()):
    lane = lax.broadcasted_iota(jnp.int32, (TILE, 2 * S), 1)
    row = lax.broadcasted_iota(jnp.int32, (TILE, 2 * S), 0)
    rest = jnp.zeros((TILE, 2 * S), F32)
    for k, value in enumerate(sums):
        rest = jnp.where((row == 0) & (lane == k), value, rest)
    return jnp.concatenate([products[:TILE], products[TILE:], rest, rest], axis=1)


def unpack(tile):
    whole = jnp.concatenate([tile[:, : 2 * S], tile[:, 2 * S : 4 * S]], axis=0)
    return whole[:, :S], whole[:, S:], tile[:, 4 * S :]


def total(ref, first=0, last=None):
    value = ref[0, first:last]
    for k in range(1, ref.shape[0]):
        value = value + ref[k, first:last]
    image = jnp.concatenate([value[0:S], value[S : 2 * S]], axis=1)
    return image, value[2 * S :]


def entire(x):
    return jnp.sum(jnp.sum(x, axis=1, keepdims=True), axis=0, keepdims=True)


def fetch(blocks, held, done):
    copies = [pltpu.make_async_copy(blocks.at[i], held.at[i], done.at[i]) for i in range(16)]
    for copy in copies:
        copy.start()
    return copies


def prepare_body(source, counts, packed, blocks, done):
    copies = fetch(source, blocks, done)
    for i in range(16):
        copies[i].wait()
        for k in range(2):
            keep = (k < counts[0, i]).astype(F32)
            high, low = halves((blocks[i, k] * keep).T)
            packed[i, k * BS : (k + 1) * BS, 0:BS] = high
            packed[i, k * BS : (k + 1) * BS, BS : 2 * BS] = low


def product_body(own, peer, packed, cols, core, out):
    me = core[0]
    for i in range(16):
        picked = []
        for k in range(2):
            col = cols[k, i]
            m = col // 4
            b = pl.multiple_of((col % 2) * S, S)
            here = own[m, pl.ds(b, S), :]
            there = peer[m, pl.ds(b, S), :]
            picked.append(jnp.where((col // 2) % 2 == me, here, there))
        high, low = halves(jnp.concatenate(picked, axis=1))
        result = bdot(jnp.concatenate([high, low], axis=0), packed[i])
        result = (result[:S, :BS] + result[:S, BS:]) + (result[S:, :BS] + result[S:, BS:])
        out[i // 2, (i % 2) * S : (i % 2 + 1) * S] = result
    if own.shape[1] > 2 * S:
        tile, tile2 = own[0, 2 * S :], peer[0, 2 * S :]
        for m in range(1, 16):
            tile = tile + own[m, 2 * S :]
            tile2 = tile2 + peer[m, 2 * S :]
        for c in range(8):
            out[c, 2 * S :] = tile + tile2


def first_body(parts, shadow, diag, image, message):
    value, _ = total(parts)
    s = shadow[...]
    v = value + diag[...] * s
    image[...] = v
    spread(message, v, pack(grams(s, jnp.concatenate([v, s], axis=0))))


def lead_step(parts, diag, image, forward, residual):
    value, tile = total(parts)
    v = image[...]
    z = value + diag[...] * v
    matrix, right, _ = unpack(tile)
    alpha = solve(matrix, right)
    q = residual[...] - mix(v, alpha)
    t = forward[...] - mix(z, alpha)
    return matrix, alpha, z, q, t


def lead_body(
    parts, shadow, diag, image, forward, residual, z_out, q_out, t_out, alpha_out, matrix_out, message
):
    matrix, alpha, z, q, t = lead_step(parts, diag, image, forward, residual)
    z_out[...] = z
    q_out[...] = q
    t_out[...] = t
    alpha_out[...] = alpha
    matrix_out[...] = matrix
    products = grams(shadow[...], jnp.concatenate([t, t], axis=0))
    spread(message, t, pack(products, (entire(t * t), entire(t * q))))


def lead_rest_body(matrix, alpha, direction, *rest):
    solution, (inverse_out, x_out) = rest[:-2], rest[-2:]
    row = lax.broadcasted_iota(jnp.int32, (S, S), 0)
    col = lax.broadcasted_iota(jnp.int32, (S, S), 1)
    inverse_out[...] = solve(matrix[...], (row == col).astype(F32))
    x = mix(direction[...], alpha[...])
    x_out[...] = x + solution[0][...] if solution else x


def follow_body(
    parts, shadow, diag, image, z, q, t, inverse, v_out, f_out, r_out, beta_out, omega_out, message
):
    value, tile = total(parts)
    middle = t[...]
    f = value + diag[...] * middle
    cross, _, sums = unpack(tile)
    omega = sums[0:1, 1:2] / sums[0:1, 0:1]
    beta = -dot(inverse[...], cross)
    residual = q[...] - omega * middle
    y = f + mix(z[...], beta)
    image_new = (middle + mix(image[...], beta)) - omega * y
    v_out[...] = image_new
    f_out[...] = f
    r_out[...] = residual
    beta_out[...] = beta
    omega_out[...] = jnp.broadcast_to(omega, omega_out.shape)
    products = grams(shadow[...], jnp.concatenate([image_new, residual], axis=0))
    spread(message, image_new, pack(products))


def follow_rest_body(t, f, r, beta, omega, image, direction, q, x, forward_out, p_out, x_out):
    o = omega[0:1, 0:1]
    forward_out[...] = t[...] - o * f[...]
    p_out[...] = r[...] + mix(direction[...] - o * image[...], beta[...])
    x_out[...] = x[...] + o * q[...]


def last_body(parts, diag, image, forward, residual, q_out, alpha_out, sums):
    _, alpha, _, q, t = lead_step(parts, diag, image, forward, residual)
    q_out[...] = q
    alpha_out[...] = alpha
    lane = lax.broadcasted_iota(jnp.int32, (1, BS), 1)
    sums[...] = jnp.where(lane == 0, entire(t * t), jnp.where(lane == 1, entire(t * q), 0.0))


def last_rest_body(alpha, direction, x, x_out):
    x_out[...] = x[...] + mix(direction[...], alpha[...])


def join_body(mine, theirs, out):
    out[...] = jnp.broadcast_to((mine[...] + theirs[...])[None], out.shape)


def end_body(sums, x, q, out):
    value = jnp.sum(sums[...], axis=0, keepdims=True)
    omega = value[0:1, 1:2] / value[0:1, 0:1]
    out[...] = x[...] + omega * q[...]


def per_device(rhs, diagonal, blocks, block_cols, counts):
    core = lax.axis_index("core").astype(jnp.int32).reshape(1)
    block_cols = block_cols.T
    counts = counts.T
    shadow = rhs.T
    diag = diagonal.reshape(1, 2 * BS)
    vec = sds(S, 2 * BS)
    small = sds(S, S)
    message = sds(16, 2 * S + TILE, BS)

    swap = [(0, 1), (1, 0)]

    def among(x):
        return lax.all_to_all(x, ("x", "z"), 0, 0, tiled=True)

    def across(x):
        return lax.all_to_all(x, "cols", 0, 0, tiled=True)

    def product(own):
        peer = lax.ppermute(own, "core", swap)
        out = call(
            product_body, sds(8, own.shape[1], BS), [VMEM, VMEM, VMEM, SMEM, SMEM],
            own, peer, packed, block_cols, core,
        )
        return across(out)

    held = [pltpu.VMEM((16, 2, BS, BS), F32), pltpu.SemaphoreType.DMA((16,))]
    piece = jnp.concatenate([shadow[:, :BS], shadow[:, BS:]], axis=0)
    own = among(jnp.broadcast_to(piece[None], (16, 2 * S, BS)))
    packed = call(
        prepare_body, sds(16, 2 * BS, 2 * BS, dtype=jnp.bfloat16), [HBM, SMEM],
        blocks, counts, scratch=held,
    )
    parts = product(own)
    v, msg = call(first_body, (vec, message), [VMEM] * 3, parts, shadow, diag)
    f, r, p, x = v, shadow, shadow, ()
    parts = product(among(msg))
    for _ in range(1, ITERS):
        z, q, t, alpha, matrix, msg = call(
            lead_body, (vec, vec, vec, small, small, message), [VMEM] * 6,
            parts, shadow, diag, v, f, r,
        )
        own = among(msg)
        inverse, x = call(lead_rest_body, (small, vec), [VMEM] * (3 + len(x)), matrix, alpha, p, *x)
        parts = product(own)
        image = v
        v, half, r, beta, omega, msg = call(
            follow_body, (vec, vec, vec, small, sds(1, BS), message), [VMEM] * 8,
            parts, shadow, diag, image, z, q, t, inverse,
        )
        own = among(msg)
        f, p, x = call(
            follow_rest_body, (vec, vec, vec), [VMEM] * 9,
            t, half, r, beta, omega, image, p, q, x,
        )
        parts = product(own)
        x = (x,)
    q, alpha, sums = call(last_body, (vec, small, sds(1, BS)), [VMEM] * 5, parts, diag, v, f, r)
    theirs = lax.ppermute(sums, "core", swap)
    x = call(last_rest_body, vec, [VMEM] * 3, alpha, p, *x)
    sums = call(join_body, sds(128, 1, BS), [VMEM] * 2, sums, theirs)
    sums = lax.all_to_all(sums, ("x", "z", "cols"), 0, 0, tiled=True)
    out = call(end_body, vec, [VMEM] * 3, sums.reshape(128, BS), x, q)
    return out.T


def solution(mesh):
    parts = ("x", "z", "core")
    mesh = jax.sharding.Mesh(mesh.devices.reshape(2, 8, 2, 8), (*parts, "cols"))
    in_specs = (
        P((*parts, "cols"), None),
        P((*parts, "cols")),
        P(parts, "cols", None, None),
        P(parts, "cols"),
        P(parts, "cols"),
    )
    out_specs = P((*parts, "cols"), None)
    return jax.shard_map(
        per_device, mesh=mesh, in_specs=in_specs, out_specs=out_specs, check_vma=False
    )
```

```python
import jax
import jax.numpy as jnp
from jax import lax
from jax.experimental import pallas as pl
from jax.experimental.pallas import tpu as pltpu
from jax.sharding import PartitionSpec as P


ITERS = 4
S = 16
BS = 128
F32 = jnp.float32
HI = lax.Precision.HIGHEST
VMEM = pl.BlockSpec(memory_space=pltpu.VMEM)
SMEM = pl.BlockSpec(memory_space=pltpu.SMEM)
HBM = pl.BlockSpec(memory_space=pltpu.HBM)
GROUP = 8
TILE = 8


def sds(*shape, dtype=F32):
    return pltpu.VMEM(shape, dtype)


def call(body, outs, specs, *args, scratch=()):
    args = [
        a if spec is SMEM else pltpu.with_memory_space_constraint(a, spec.memory_space)
        for a, spec in zip(args, specs)
    ]
    return pl.pallas_call(
        body,
        out_shape=outs,
        in_specs=specs,
        out_specs=tuple(VMEM for _ in outs) if isinstance(outs, tuple) else VMEM,
        scratch_shapes=scratch,
        compiler_params=pltpu.CompilerParams(vmem_limit_bytes=8 << 20),
    )(*args)


def dot(a, b, contract=((1,), (0,))):
    return lax.dot_general(a, b, (contract, ((), ())), precision=HI, preferred_element_type=F32)


def bdot(a, b):
    return lax.dot_general(a, b, (((1,), (0,)), ((), ())), preferred_element_type=F32)


def halves(x):
    high = x.astype(jnp.bfloat16)
    return high, (x - high.astype(F32)).astype(jnp.bfloat16)


def spread(ref, value, tile):
    for k in range(ref.shape[0]):
        ref[k, 0:S] = value[:, :BS]
        ref[k, S : 2 * S] = value[:, BS:]
        ref[k, 2 * S : 2 * S + TILE] = tile


def solve(matrix, right):
    joined = jnp.concatenate([matrix, right], axis=1)
    row = lax.broadcasted_iota(jnp.int32, joined.shape, 0)

    def step(i, x, column):
        pivot = x[i : i + 1, :] / column[i : i + 1, :]
        return jnp.where(row == i, pivot, x - column * pivot)

    for first in range(0, S, GROUP):
        last = first + GROUP
        columns = {
            j: jnp.broadcast_to(joined[:, j : j + 1], joined.shape) for j in range(first, last)
        }
        for i in range(first, last):
            joined = step(i, joined, columns[i])
            for j in range(i + 1, last):
                columns[j] = step(i, columns[j], columns[i])
    return joined[:, S:]


def mix(vectors, small):
    return dot(small.T, vectors)


def grams(left, right):
    return dot(left, right, ((1,), (1,)))


def pack(products, sums=()):
    lane = lax.broadcasted_iota(jnp.int32, (TILE, 2 * S), 1)
    row = lax.broadcasted_iota(jnp.int32, (TILE, 2 * S), 0)
    rest = jnp.zeros((TILE, 2 * S), F32)
    for k, value in enumerate(sums):
        rest = jnp.where((row == 0) & (lane == k), value, rest)
    return jnp.concatenate([products[:TILE], products[TILE:], rest, rest], axis=1)


def unpack(tile):
    whole = jnp.concatenate([tile[:, : 2 * S], tile[:, 2 * S : 4 * S]], axis=0)
    return whole[:, :S], whole[:, S:], tile[:, 4 * S :]


def total(ref, first=0, last=None):
    value = ref[0, first:last]
    for k in range(1, ref.shape[0]):
        value = value + ref[k, first:last]
    image = jnp.concatenate([value[0:S], value[S : 2 * S]], axis=1)
    return image, value[2 * S :]


def entire(x):
    return jnp.sum(jnp.sum(x, axis=1, keepdims=True), axis=0, keepdims=True)


def fetch(blocks, held, done):
    copies = [pltpu.make_async_copy(blocks.at[i], held.at[i], done.at[i]) for i in range(16)]
    for copy in copies:
        copy.start()
    return copies


def prepare_body(source, counts, packed, blocks, done):
    copies = fetch(source, blocks, done)
    for i in range(16):
        copies[i].wait()
        for k in range(2):
            keep = (k < counts[0, i]).astype(F32)
            high, low = halves((blocks[i, k] * keep).T)
            packed[i, k * BS : (k + 1) * BS, 0:BS] = high
            packed[i, k * BS : (k + 1) * BS, BS : 2 * BS] = low


def product_body(own, peer, packed, cols, core, out):
    me = core[0]
    for i in range(16):
        picked = []
        for k in range(2):
            col = cols[k, i]
            m = col // 4
            b = pl.multiple_of((col % 2) * S, S)
            here = own[m, pl.ds(b, S), :]
            there = peer[m, pl.ds(b, S), :]
            picked.append(jnp.where((col // 2) % 2 == me, here, there))
        high, low = halves(jnp.concatenate(picked, axis=1))
        result = bdot(jnp.concatenate([high, low], axis=0), packed[i])
        result = (result[:S, :BS] + result[:S, BS:]) + (result[S:, :BS] + result[S:, BS:])
        out[i // 2, (i % 2) * S : (i % 2 + 1) * S] = result
    if own.shape[1] > 2 * S:
        tile, tile2 = own[0, 2 * S :], peer[0, 2 * S :]
        for m in range(1, 16):
            tile = tile + own[m, 2 * S :]
            tile2 = tile2 + peer[m, 2 * S :]
        for c in range(8):
            out[c, 2 * S :] = tile + tile2


def first_body(parts, shadow, diag, image, message):
    value, _ = total(parts)
    s = shadow[...]
    v = value + diag[...] * s
    image[...] = v
    spread(message, v, pack(grams(s, jnp.concatenate([v, s], axis=0))))


def lead_step(parts, diag, image, forward, residual):
    value, tile = total(parts)
    v = image[...]
    z = value + diag[...] * v
    matrix, right, _ = unpack(tile)
    alpha = solve(matrix, right)
    q = residual[...] - mix(v, alpha)
    t = forward[...] - mix(z, alpha)
    return matrix, alpha, z, q, t


def lead_body(
    parts, shadow, diag, image, forward, residual, z_out, q_out, t_out, alpha_out, matrix_out, message
):
    matrix, alpha, z, q, t = lead_step(parts, diag, image, forward, residual)
    z_out[...] = z
    q_out[...] = q
    t_out[...] = t
    alpha_out[...] = alpha
    matrix_out[...] = matrix
    products = grams(shadow[...], jnp.concatenate([t, t], axis=0))
    spread(message, t, pack(products, (entire(t * t), entire(t * q))))


def lead_rest_body(matrix, alpha, direction, *rest):
    solution, (inverse_out, x_out) = rest[:-2], rest[-2:]
    row = lax.broadcasted_iota(jnp.int32, (S, S), 0)
    col = lax.broadcasted_iota(jnp.int32, (S, S), 1)
    inverse_out[...] = solve(matrix[...], (row == col).astype(F32))
    x = mix(direction[...], alpha[...])
    x_out[...] = x + solution[0][...] if solution else x


def follow_body(
    parts, shadow, diag, image, z, q, t, inverse, v_out, f_out, r_out, beta_out, omega_out, message
):
    value, tile = total(parts)
    middle = t[...]
    f = value + diag[...] * middle
    cross, _, sums = unpack(tile)
    omega = sums[0:1, 1:2] / sums[0:1, 0:1]
    beta = -dot(inverse[...], cross)
    residual = q[...] - omega * middle
    y = f + mix(z[...], beta)
    image_new = (middle + mix(image[...], beta)) - omega * y
    v_out[...] = image_new
    f_out[...] = f
    r_out[...] = residual
    beta_out[...] = beta
    omega_out[...] = jnp.broadcast_to(omega, omega_out.shape)
    products = grams(shadow[...], jnp.concatenate([image_new, residual], axis=0))
    spread(message, image_new, pack(products))


def follow_rest_body(t, f, r, beta, omega, image, direction, q, x, forward_out, p_out, x_out):
    o = omega[0:1, 0:1]
    forward_out[...] = t[...] - o * f[...]
    p_out[...] = r[...] + mix(direction[...] - o * image[...], beta[...])
    x_out[...] = x[...] + o * q[...]


def last_body(parts, diag, image, forward, residual, q_out, alpha_out, sums):
    _, alpha, _, q, t = lead_step(parts, diag, image, forward, residual)
    q_out[...] = q
    alpha_out[...] = alpha
    lane = lax.broadcasted_iota(jnp.int32, (1, BS), 1)
    sums[...] = jnp.where(lane == 0, entire(t * t), jnp.where(lane == 1, entire(t * q), 0.0))


def end_body(sums, alpha, direction, x, q, out):
    value = jnp.sum(sums[...], axis=0, keepdims=True)
    omega = value[0:1, 1:2] / value[0:1, 0:1]
    out[...] = x[...] + mix(direction[...], alpha[...]) + omega * q[...]


def per_device(rhs, diagonal, blocks, block_cols, counts):
    core = lax.axis_index("core").astype(jnp.int32).reshape(1)
    block_cols = block_cols.T
    counts = counts.T
    shadow = rhs.T
    diag = diagonal.reshape(1, 2 * BS)
    vec = sds(S, 2 * BS)
    small = sds(S, S)
    message = sds(16, 2 * S + TILE, BS)

    def among(x):
        return lax.all_to_all(x, ("x", "z"), 0, 0, tiled=True)

    def across(x):
        return lax.all_to_all(x, "cols", 0, 0, tiled=True)

    def exchange(own):
        return lax.ppermute(own, "core", [(0, 1), (1, 0)])

    def product(own, peer):
        out = call(
            product_body, sds(8, own.shape[1], BS), [VMEM, VMEM, VMEM, SMEM, SMEM],
            own, peer, packed, block_cols, core,
        )
        return across(out)

    held = [pltpu.VMEM((16, 2, BS, BS), F32), pltpu.SemaphoreType.DMA((16,))]
    piece = jnp.concatenate([shadow[:, :BS], shadow[:, BS:]], axis=0)
    own = among(jnp.broadcast_to(piece[None], (16, 2 * S, BS)))
    packed = call(
        prepare_body, sds(16, 2 * BS, 2 * BS, dtype=jnp.bfloat16), [HBM, SMEM],
        blocks, counts, scratch=held,
    )
    parts = product(own, exchange(own))
    v, msg = call(first_body, (vec, message), [VMEM] * 3, parts, shadow, diag)
    f, r, p, x = v, shadow, shadow, ()
    own = among(msg)
    parts = product(own, exchange(own))
    for _ in range(1, ITERS):
        z, q, t, alpha, matrix, msg = call(
            lead_body, (vec, vec, vec, small, small, message), [VMEM] * 6,
            parts, shadow, diag, v, f, r,
        )
        own = among(msg)
        peer = exchange(own)
        inverse, x = call(lead_rest_body, (small, vec), [VMEM] * (3 + len(x)), matrix, alpha, p, *x)
        parts = product(own, peer)
        image = v
        v, half, r, beta, omega, msg = call(
            follow_body, (vec, vec, vec, small, sds(1, BS), message), [VMEM] * 8,
            parts, shadow, diag, image, z, q, t, inverse,
        )
        own = among(msg)
        peer = exchange(own)
        f, p, x = call(
            follow_rest_body, (vec, vec, vec), [VMEM] * 9,
            t, half, r, beta, omega, image, p, q, x,
        )
        parts = product(own, peer)
        x = (x,)
    q, alpha, sums = call(last_body, (vec, small, sds(1, BS)), [VMEM] * 5, parts, diag, v, f, r)
    everyone = 2 * 16 * 8
    sums = jnp.broadcast_to(sums[None], (everyone, 1, BS))
    sums = lax.all_to_all(sums, ("x", "z", "core", "cols"), 0, 0, tiled=True)
    out = call(end_body, vec, [VMEM] * 5, sums.reshape(everyone, BS), alpha, p, x[0], q)
    return out.T


def solution(mesh):
    parts = ("x", "z", "core")
    mesh = jax.sharding.Mesh(mesh.devices.reshape(2, 8, 2, 8), (*parts, "cols"))
    in_specs = (
        P((*parts, "cols"), None),
        P((*parts, "cols")),
        P(parts, "cols", None, None),
        P(parts, "cols"),
        P(parts, "cols"),
    )
    out_specs = P((*parts, "cols"), None)
    return jax.shard_map(
        per_device, mesh=mesh, in_specs=in_specs, out_specs=out_specs, check_vma=False
    )
```

```python
import jax
import jax.numpy as jnp
from jax import lax
from jax.experimental import pallas as pl
from jax.experimental.pallas import tpu as pltpu
from jax.sharding import PartitionSpec as P


ITERS = 4
S = 16
BS = 128
F32 = jnp.float32
HI = lax.Precision.HIGHEST
VMEM = pl.BlockSpec(memory_space=pltpu.VMEM)
SMEM = pl.BlockSpec(memory_space=pltpu.SMEM)
HBM = pl.BlockSpec(memory_space=pltpu.HBM)
GROUP = 8
TILE = 8


def sds(*shape, dtype=F32):
    return pltpu.VMEM(shape, dtype)


def call(body, outs, specs, *args, scratch=()):
    args = [
        a if spec is SMEM else pltpu.with_memory_space_constraint(a, spec.memory_space)
        for a, spec in zip(args, specs)
    ]
    return pl.pallas_call(
        body,
        out_shape=outs,
        in_specs=specs,
        out_specs=tuple(VMEM for _ in outs) if isinstance(outs, tuple) else VMEM,
        scratch_shapes=scratch,
        compiler_params=pltpu.CompilerParams(vmem_limit_bytes=8 << 20),
    )(*args)


def dot(a, b, contract=((1,), (0,))):
    return lax.dot_general(a, b, (contract, ((), ())), precision=HI, preferred_element_type=F32)


def bdot(a, b):
    return lax.dot_general(a, b, (((1,), (0,)), ((), ())), preferred_element_type=F32)


def halves(x):
    high = x.astype(jnp.bfloat16)
    return high, (x - high.astype(F32)).astype(jnp.bfloat16)


def spread(ref, value, tile):
    for k in range(ref.shape[0]):
        ref[k, 0:S] = value[:, :BS]
        ref[k, S : 2 * S] = value[:, BS:]
        ref[k, 2 * S : 2 * S + TILE] = tile


def solve(matrix, right):
    joined = jnp.concatenate([matrix, right], axis=1)
    row = lax.broadcasted_iota(jnp.int32, joined.shape, 0)

    def step(i, x, column):
        pivot = x[i : i + 1, :] / column[i : i + 1, :]
        return jnp.where(row == i, pivot, x - column * pivot)

    for first in range(0, S, GROUP):
        last = first + GROUP
        columns = {
            j: jnp.broadcast_to(joined[:, j : j + 1], joined.shape) for j in range(first, last)
        }
        for i in range(first, last):
            joined = step(i, joined, columns[i])
            for j in range(i + 1, last):
                columns[j] = step(i, columns[j], columns[i])
    return joined[:, S:]


def mix(vectors, small):
    return dot(small.T, vectors)


def grams(left, right):
    return dot(left, right, ((1,), (1,)))


def pack(products, sums=()):
    lane = lax.broadcasted_iota(jnp.int32, (TILE, 2 * S), 1)
    row = lax.broadcasted_iota(jnp.int32, (TILE, 2 * S), 0)
    rest = jnp.zeros((TILE, 2 * S), F32)
    for k, value in enumerate(sums):
        rest = jnp.where((row == 0) & (lane == k), value, rest)
    return jnp.concatenate([products[:TILE], products[TILE:], rest, rest], axis=1)


def unpack(tile):
    whole = jnp.concatenate([tile[:, : 2 * S], tile[:, 2 * S : 4 * S]], axis=0)
    return whole[:, :S], whole[:, S:], tile[:, 4 * S :]


def total(ref, first=0, last=None):
    value = ref[0, first:last]
    for k in range(1, ref.shape[0]):
        value = value + ref[k, first:last]
    image = jnp.concatenate([value[0:S], value[S : 2 * S]], axis=1)
    return image, value[2 * S :]


def entire(x):
    return jnp.sum(jnp.sum(x, axis=1, keepdims=True), axis=0, keepdims=True)


def fetch(blocks, held, done):
    copies = [pltpu.make_async_copy(blocks.at[i], held.at[i], done.at[i]) for i in range(16)]
    for copy in copies:
        copy.start()
    return copies


def prepare_body(source, counts, packed, blocks, done):
    copies = fetch(source, blocks, done)
    for i in range(16):
        copies[i].wait()
        for k in range(2):
            keep = (k < counts[0, i]).astype(F32)
            high, low = halves((blocks[i, k] * keep).T)
            packed[i, k * BS : (k + 1) * BS, 0:BS] = high
            packed[i, k * BS : (k + 1) * BS, BS : 2 * BS] = low


def product_body(own, peer, packed, cols, core, out):
    me = core[0]
    for i in range(16):
        picked = []
        for k in range(2):
            col = cols[k, i]
            m = col >> 2
            b = pl.multiple_of((col & 1) * S, S)
            here = own[m, pl.ds(b, S), :]
            there = peer[m, pl.ds(b, S), :]
            picked.append(jnp.where((col >> 1) & 1 == me, here, there))
        high, low = halves(jnp.concatenate(picked, axis=1))
        result = bdot(jnp.concatenate([high, low], axis=0), packed[i])
        result = (result[:S, :BS] + result[:S, BS:]) + (result[S:, :BS] + result[S:, BS:])
        out[i // 2, (i % 2) * S : (i % 2 + 1) * S] = result
    if own.shape[1] > 2 * S:
        tile, tile2 = own[0, 2 * S :], peer[0, 2 * S :]
        for m in range(1, 16):
            tile = tile + own[m, 2 * S :]
            tile2 = tile2 + peer[m, 2 * S :]
        for c in range(8):
            out[c, 2 * S :] = tile + tile2


def start_body(shadow, message):
    value = shadow[...]
    for k in range(message.shape[0]):
        message[k, 0:S] = value[:, :BS]
        message[k, S:] = value[:, BS:]


def first_body(parts, shadow, diag, image, message):
    value, _ = total(parts)
    s = shadow[...]
    v = value + diag[...] * s
    image[...] = v
    spread(message, v, pack(grams(s, jnp.concatenate([v, s], axis=0))))


def lead_step(parts, diag, image, forward, residual):
    value, tile = total(parts)
    v = image[...]
    z = value + diag[...] * v
    matrix, right, _ = unpack(tile)
    alpha = solve(matrix, right)
    q = residual[...] - mix(v, alpha)
    t = forward[...] - mix(z, alpha)
    return matrix, alpha, z, q, t


def lead_body(
    parts, shadow, diag, image, forward, residual, z_out, q_out, t_out, alpha_out, matrix_out, message
):
    matrix, alpha, z, q, t = lead_step(parts, diag, image, forward, residual)
    z_out[...] = z
    q_out[...] = q
    t_out[...] = t
    alpha_out[...] = alpha
    matrix_out[...] = matrix
    products = grams(shadow[...], jnp.concatenate([t, t], axis=0))
    spread(message, t, pack(products, (entire(t * t), entire(t * q))))


def lead_rest_body(matrix, alpha, direction, *rest):
    solution, (inverse_out, x_out) = rest[:-2], rest[-2:]
    row = lax.broadcasted_iota(jnp.int32, (S, S), 0)
    col = lax.broadcasted_iota(jnp.int32, (S, S), 1)
    inverse_out[...] = solve(matrix[...], (row == col).astype(F32))
    x = mix(direction[...], alpha[...])
    x_out[...] = x + solution[0][...] if solution else x


def follow_body(
    parts, shadow, diag, image, z, q, t, inverse, v_out, f_out, r_out, beta_out, omega_out, message
):
    value, tile = total(parts)
    middle = t[...]
    f = value + diag[...] * middle
    cross, _, sums = unpack(tile)
    omega = sums[0:1, 1:2] / sums[0:1, 0:1]
    beta = -dot(inverse[...], cross)
    residual = q[...] - omega * middle
    y = f + mix(z[...], beta)
    image_new = (middle + mix(image[...], beta)) - omega * y
    v_out[...] = image_new
    f_out[...] = f
    r_out[...] = residual
    beta_out[...] = beta
    omega_out[...] = jnp.broadcast_to(omega, omega_out.shape)
    products = grams(shadow[...], jnp.concatenate([image_new, residual], axis=0))
    spread(message, image_new, pack(products))


def follow_rest_body(t, f, r, beta, omega, image, direction, q, x, forward_out, p_out, x_out):
    o = omega[0:1, 0:1]
    forward_out[...] = t[...] - o * f[...]
    p_out[...] = r[...] + mix(direction[...] - o * image[...], beta[...])
    x_out[...] = x[...] + o * q[...]


def last_body(parts, diag, image, forward, residual, q_out, alpha_out, sums):
    _, alpha, _, q, t = lead_step(parts, diag, image, forward, residual)
    q_out[...] = q
    alpha_out[...] = alpha
    lane = lax.broadcasted_iota(jnp.int32, (1, BS), 1)
    sums[...] = jnp.where(lane == 0, entire(t * t), jnp.where(lane == 1, entire(t * q), 0.0))


def end_body(sums, alpha, direction, x, q, out):
    value = jnp.sum(sums[...], axis=0, keepdims=True)
    omega = value[0:1, 1:2] / value[0:1, 0:1]
    out[...] = x[...] + mix(direction[...], alpha[...]) + omega * q[...]


def per_device(rhs, diagonal, blocks, block_cols, counts):
    core = lax.axis_index("core").astype(jnp.int32).reshape(1)
    block_cols = block_cols.T
    counts = counts.T
    shadow = rhs.T
    diag = diagonal.reshape(1, 2 * BS)
    vec = sds(S, 2 * BS)
    small = sds(S, S)
    message = sds(16, 2 * S + TILE, BS)

    def among(x):
        return lax.all_to_all(x, ("x", "z"), 0, 0, tiled=True)

    def across(x):
        return lax.all_to_all(x, "cols", 0, 0, tiled=True)

    def exchange(own):
        return lax.ppermute(own, "core", [(0, 1), (1, 0)])

    def product(own, peer):
        out = call(
            product_body, sds(8, own.shape[1], BS), [VMEM, VMEM, VMEM, SMEM, SMEM],
            own, peer, packed, block_cols, core,
        )
        return across(out)

    held = [pltpu.VMEM((16, 2, BS, BS), F32), pltpu.SemaphoreType.DMA((16,))]
    msg = call(start_body, jax.ShapeDtypeStruct((16, 2 * S, BS), F32), [VMEM], shadow)
    own = among(msg)
    packed = call(
        prepare_body, sds(16, 2 * BS, 2 * BS, dtype=jnp.bfloat16), [HBM, SMEM],
        blocks, counts, scratch=held,
    )
    parts = product(own, exchange(own))
    v, msg = call(first_body, (vec, message), [VMEM] * 3, parts, shadow, diag)
    f, r, p, x = v, shadow, shadow, ()
    own = among(msg)
    parts = product(own, exchange(own))
    for _ in range(1, ITERS):
        z, q, t, alpha, matrix, msg = call(
            lead_body, (vec, vec, vec, small, small, message), [VMEM] * 6,
            parts, shadow, diag, v, f, r,
        )
        own = among(msg)
        peer = exchange(own)
        inverse, x = call(lead_rest_body, (small, vec), [VMEM] * (3 + len(x)), matrix, alpha, p, *x)
        parts = product(own, peer)
        image = v
        v, half, r, beta, omega, msg = call(
            follow_body, (vec, vec, vec, small, sds(1, BS), message), [VMEM] * 8,
            parts, shadow, diag, image, z, q, t, inverse,
        )
        own = among(msg)
        peer = exchange(own)
        f, p, x = call(
            follow_rest_body, (vec, vec, vec), [VMEM] * 9,
            t, half, r, beta, omega, image, p, q, x,
        )
        parts = product(own, peer)
        x = (x,)
    q, alpha, sums = call(last_body, (vec, small, sds(1, BS)), [VMEM] * 5, parts, diag, v, f, r)
    everyone = 2 * 16 * 8
    sums = jnp.broadcast_to(sums[None], (everyone, 1, BS))
    sums = lax.all_to_all(sums, ("x", "z", "core", "cols"), 0, 0, tiled=True)
    out = call(
        end_body, jax.ShapeDtypeStruct((S, 2 * BS), F32), [VMEM] * 5, sums.reshape(everyone, BS), alpha, p, x[0], q
    )
    return out.T


def solution(mesh):
    parts = ("x", "z", "core")
    mesh = jax.sharding.Mesh(mesh.devices.reshape(2, 8, 2, 8), (*parts, "cols"))
    in_specs = (
        P((*parts, "cols"), None),
        P((*parts, "cols")),
        P(parts, "cols", None, None),
        P(parts, "cols"),
        P(parts, "cols"),
    )
    out_specs = P((*parts, "cols"), None)
    return jax.shard_map(
        per_device, mesh=mesh, in_specs=in_specs, out_specs=out_specs, check_vma=False
    )
```

```python
import jax
import jax.numpy as jnp
from jax import lax
from jax.experimental import pallas as pl
from jax.experimental.pallas import tpu as pltpu
from jax.sharding import PartitionSpec as P


ITERS = 4
S = 16
BS = 128
F32 = jnp.float32
HI = lax.Precision.HIGHEST
VMEM = pl.BlockSpec(memory_space=pltpu.VMEM)
SMEM = pl.BlockSpec(memory_space=pltpu.SMEM)
HBM = pl.BlockSpec(memory_space=pltpu.HBM)
GROUP = 8
TILE = 8


def sds(*shape, dtype=F32):
    return pltpu.VMEM(shape, dtype)


def call(body, outs, specs, *args, scratch=()):
    args = [
        a if spec is SMEM else pltpu.with_memory_space_constraint(a, spec.memory_space)
        for a, spec in zip(args, specs)
    ]
    return pl.pallas_call(
        body,
        out_shape=outs,
        in_specs=specs,
        out_specs=tuple(VMEM for _ in outs) if isinstance(outs, tuple) else VMEM,
        scratch_shapes=scratch,
        compiler_params=pltpu.CompilerParams(vmem_limit_bytes=8 << 20),
    )(*args)


def dot(a, b, contract=((1,), (0,))):
    return lax.dot_general(a, b, (contract, ((), ())), precision=HI, preferred_element_type=F32)


def bdot(a, b):
    return lax.dot_general(a, b, (((1,), (0,)), ((), ())), preferred_element_type=F32)


def halves(x):
    high = x.astype(jnp.bfloat16)
    return high, (x - high.astype(F32)).astype(jnp.bfloat16)


def spread(ref, value, tile):
    for k in range(ref.shape[0]):
        ref[k, 0:S] = value[:, :BS]
        ref[k, S : 2 * S] = value[:, BS:]
        ref[k, 2 * S : 2 * S + TILE] = tile


def solve(matrix, right):
    joined = jnp.concatenate([matrix, right], axis=1)
    row = lax.broadcasted_iota(jnp.int32, joined.shape, 0)

    def step(i, x, column):
        pivot = x[i : i + 1, :] / column[i : i + 1, :]
        return jnp.where(row == i, pivot, x - column * pivot)

    for first in range(0, S, GROUP):
        last = first + GROUP
        columns = {
            j: jnp.broadcast_to(joined[:, j : j + 1], joined.shape) for j in range(first, last)
        }
        for i in range(first, last):
            joined = step(i, joined, columns[i])
            for j in range(i + 1, last):
                columns[j] = step(i, columns[j], columns[i])
    return joined[:, S:]


def mix(vectors, small):
    return dot(small.T, vectors)


def grams(left, right):
    return dot(left, right, ((1,), (1,)))


def pack(products, sums=()):
    lane = lax.broadcasted_iota(jnp.int32, (TILE, 2 * S), 1)
    row = lax.broadcasted_iota(jnp.int32, (TILE, 2 * S), 0)
    rest = jnp.zeros((TILE, 2 * S), F32)
    for k, value in enumerate(sums):
        rest = jnp.where((row == 0) & (lane == k), value, rest)
    return jnp.concatenate([products[:TILE], products[TILE:], rest, rest], axis=1)


def unpack(tile):
    whole = jnp.concatenate([tile[:, : 2 * S], tile[:, 2 * S : 4 * S]], axis=0)
    return whole[:, :S], whole[:, S:], tile[:, 4 * S :]


def total(ref, first=0, last=None):
    value = ref[0, first:last]
    for k in range(1, ref.shape[0]):
        value = value + ref[k, first:last]
    image = jnp.concatenate([value[0:S], value[S : 2 * S]], axis=1)
    return image, value[2 * S :]


def entire(x):
    return jnp.sum(jnp.sum(x, axis=1, keepdims=True), axis=0, keepdims=True)


def fetch(blocks, held, done):
    copies = [pltpu.make_async_copy(blocks.at[i], held.at[i], done.at[i]) for i in range(16)]
    for copy in copies:
        copy.start()
    return copies


def prepare_body(source, counts, packed, blocks, done):
    copies = fetch(source, blocks, done)
    for i in range(16):
        copies[i].wait()
        for k in range(2):
            keep = (k < counts[0, i]).astype(F32)
            high, low = halves((blocks[i, k] * keep).T)
            packed[i, k * BS : (k + 1) * BS, 0:BS] = high
            packed[i, k * BS : (k + 1) * BS, BS : 2 * BS] = low


def product_body(own, peer, packed, cols, core, out):
    me = core[0]
    for i in range(16):
        picked = []
        for k in range(2):
            col = cols[k, i]
            m = (col >> 5) * 8 + ((col >> 2) * 3 & 7)
            b = pl.multiple_of((col & 1) * S, S)
            here = own[m, pl.ds(b, S), :]
            there = peer[m, pl.ds(b, S), :]
            picked.append(jnp.where((col >> 1) & 1 == me, here, there))
        high, low = halves(jnp.concatenate(picked, axis=1))
        result = bdot(jnp.concatenate([high, low], axis=0), packed[i])
        result = (result[:S, :BS] + result[:S, BS:]) + (result[S:, :BS] + result[S:, BS:])
        out[i // 2, (i % 2) * S : (i % 2 + 1) * S] = result
    if own.shape[1] > 2 * S:
        tile, tile2 = own[0, 2 * S :], peer[0, 2 * S :]
        for m in range(1, 16):
            tile = tile + own[m, 2 * S :]
            tile2 = tile2 + peer[m, 2 * S :]
        for c in range(8):
            out[c, 2 * S :] = tile + tile2


def start_body(shadow, message):
    value = shadow[...]
    for k in range(message.shape[0]):
        message[k, 0:S] = value[:, :BS]
        message[k, S:] = value[:, BS:]


def first_body(parts, shadow, diag, image, message):
    value, _ = total(parts)
    s = shadow[...]
    v = value + diag[...] * s
    image[...] = v
    spread(message, v, pack(grams(s, jnp.concatenate([v, s], axis=0))))


def lead_step(parts, diag, image, forward, residual):
    value, tile = total(parts)
    v = image[...]
    z = value + diag[...] * v
    matrix, right, _ = unpack(tile)
    alpha = solve(matrix, right)
    q = residual[...] - mix(v, alpha)
    t = forward[...] - mix(z, alpha)
    return matrix, alpha, z, q, t


def lead_body(
    parts, shadow, diag, image, forward, residual, z_out, q_out, t_out, alpha_out, matrix_out, message
):
    matrix, alpha, z, q, t = lead_step(parts, diag, image, forward, residual)
    z_out[...] = z
    q_out[...] = q
    t_out[...] = t
    alpha_out[...] = alpha
    matrix_out[...] = matrix
    products = grams(shadow[...], jnp.concatenate([t, t], axis=0))
    spread(message, t, pack(products, (entire(t * t), entire(t * q))))


def lead_rest_body(matrix, alpha, direction, *rest):
    solution, (inverse_out, x_out) = rest[:-2], rest[-2:]
    row = lax.broadcasted_iota(jnp.int32, (S, S), 0)
    col = lax.broadcasted_iota(jnp.int32, (S, S), 1)
    inverse_out[...] = solve(matrix[...], (row == col).astype(F32))
    x = mix(direction[...], alpha[...])
    x_out[...] = x + solution[0][...] if solution else x


def follow_body(
    parts, shadow, diag, image, z, q, t, inverse, v_out, f_out, r_out, beta_out, omega_out, message
):
    value, tile = total(parts)
    middle = t[...]
    f = value + diag[...] * middle
    cross, _, sums = unpack(tile)
    omega = sums[0:1, 1:2] / sums[0:1, 0:1]
    beta = -dot(inverse[...], cross)
    residual = q[...] - omega * middle
    y = f + mix(z[...], beta)
    image_new = (middle + mix(image[...], beta)) - omega * y
    v_out[...] = image_new
    f_out[...] = f
    r_out[...] = residual
    beta_out[...] = beta
    omega_out[...] = jnp.broadcast_to(omega, omega_out.shape)
    products = grams(shadow[...], jnp.concatenate([image_new, residual], axis=0))
    spread(message, image_new, pack(products))


def follow_rest_body(t, f, r, beta, omega, image, direction, q, x, forward_out, p_out, x_out):
    o = omega[0:1, 0:1]
    forward_out[...] = t[...] - o * f[...]
    p_out[...] = r[...] + mix(direction[...] - o * image[...], beta[...])
    x_out[...] = x[...] + o * q[...]


def last_body(parts, diag, image, forward, residual, q_out, alpha_out, sums):
    _, alpha, _, q, t = lead_step(parts, diag, image, forward, residual)
    q_out[...] = q
    alpha_out[...] = alpha
    lane = lax.broadcasted_iota(jnp.int32, (1, BS), 1)
    sums[...] = jnp.where(lane == 0, entire(t * t), jnp.where(lane == 1, entire(t * q), 0.0))


def end_body(sums, alpha, direction, x, q, out):
    value = jnp.sum(sums[...], axis=0, keepdims=True)
    omega = value[0:1, 1:2] / value[0:1, 0:1]
    out[...] = x[...] + mix(direction[...], alpha[...]) + omega * q[...]


def per_device(rhs, diagonal, blocks, block_cols, counts):
    core = (lax.axis_index("rows") % 2).astype(jnp.int32).reshape(1)
    groups = [[16 * (m // 8) + 2 * (3 * m % 8) + c for m in range(16)] for c in range(2)]
    partner = [(r, r ^ 1) for r in range(32)]
    block_cols = block_cols.T
    counts = counts.T
    shadow = rhs.T
    diag = diagonal.reshape(1, 2 * BS)
    vec = sds(S, 2 * BS)
    small = sds(S, S)
    message = sds(16, 2 * S + TILE, BS)

    def among(x):
        return lax.all_to_all(x, "rows", 0, 0, tiled=True, axis_index_groups=groups)

    def across(x):
        return lax.all_to_all(x, "cols", 0, 0, tiled=True)

    def exchange(own):
        return lax.ppermute(own, "rows", partner)

    def product(own, peer):
        out = call(
            product_body, sds(8, own.shape[1], BS), [VMEM, VMEM, VMEM, SMEM, SMEM],
            own, peer, packed, block_cols, core,
        )
        return across(out)

    held = [pltpu.VMEM((16, 2, BS, BS), F32), pltpu.SemaphoreType.DMA((16,))]
    msg = call(start_body, jax.ShapeDtypeStruct((16, 2 * S, BS), F32), [VMEM], shadow)
    own = among(msg)
    packed = call(
        prepare_body, sds(16, 2 * BS, 2 * BS, dtype=jnp.bfloat16), [HBM, SMEM],
        blocks, counts, scratch=held,
    )
    parts = product(own, exchange(own))
    v, msg = call(first_body, (vec, message), [VMEM] * 3, parts, shadow, diag)
    f, r, p, x = v, shadow, shadow, ()
    own = among(msg)
    parts = product(own, exchange(own))
    for _ in range(1, ITERS):
        z, q, t, alpha, matrix, msg = call(
            lead_body, (vec, vec, vec, small, small, message), [VMEM] * 6,
            parts, shadow, diag, v, f, r,
        )
        own = among(msg)
        peer = exchange(own)
        inverse, x = call(lead_rest_body, (small, vec), [VMEM] * (3 + len(x)), matrix, alpha, p, *x)
        parts = product(own, peer)
        image = v
        v, half, r, beta, omega, msg = call(
            follow_body, (vec, vec, vec, small, sds(1, BS), message), [VMEM] * 8,
            parts, shadow, diag, image, z, q, t, inverse,
        )
        own = among(msg)
        peer = exchange(own)
        f, p, x = call(
            follow_rest_body, (vec, vec, vec), [VMEM] * 9,
            t, half, r, beta, omega, image, p, q, x,
        )
        parts = product(own, peer)
        x = (x,)
    q, alpha, sums = call(last_body, (vec, small, sds(1, BS)), [VMEM] * 5, parts, diag, v, f, r)
    everyone = 2 * 16 * 8
    sums = jnp.broadcast_to(sums[None], (everyone, 1, BS))
    sums = lax.all_to_all(sums, ("rows", "cols"), 0, 0, tiled=True)
    out = call(
        end_body, jax.ShapeDtypeStruct((S, 2 * BS), F32), [VMEM] * 5, sums.reshape(everyone, BS), alpha, p, x[0], q
    )
    return out.T


def solution(mesh):
    in_specs = (
        P(("rows", "cols"), None),
        P(("rows", "cols")),
        P("rows", "cols", None, None),
        P("rows", "cols"),
        P("rows", "cols"),
    )
    out_specs = P(("rows", "cols"), None)
    return jax.shard_map(
        per_device, mesh=mesh, in_specs=in_specs, out_specs=out_specs, check_vma=False
    )
```

```python
import jax
import jax.numpy as jnp
from jax import lax
from jax.experimental import pallas as pl
from jax.experimental.pallas import tpu as pltpu
from jax.sharding import PartitionSpec as P


ITERS = 4
S = 16
BS = 128
F32 = jnp.float32
HI = lax.Precision.HIGHEST
VMEM = pl.BlockSpec(memory_space=pltpu.VMEM)
SMEM = pl.BlockSpec(memory_space=pltpu.SMEM)
HBM = pl.BlockSpec(memory_space=pltpu.HBM)
GROUP = 16
TILE = 8


def sds(*shape, dtype=F32):
    return pltpu.VMEM(shape, dtype)


def call(body, outs, specs, *args, scratch=()):
    args = [
        a if spec is SMEM else pltpu.with_memory_space_constraint(a, spec.memory_space)
        for a, spec in zip(args, specs)
    ]
    return pl.pallas_call(
        body,
        out_shape=outs,
        in_specs=specs,
        out_specs=tuple(VMEM for _ in outs) if isinstance(outs, tuple) else VMEM,
        scratch_shapes=scratch,
        compiler_params=pltpu.CompilerParams(vmem_limit_bytes=8 << 20),
    )(*args)


def dot(a, b, contract=((1,), (0,))):
    return lax.dot_general(a, b, (contract, ((), ())), precision=HI, preferred_element_type=F32)


def bdot(a, b):
    return lax.dot_general(a, b, (((1,), (0,)), ((), ())), preferred_element_type=F32)


def halves(x):
    high = x.astype(jnp.bfloat16)
    return high, (x - high.astype(F32)).astype(jnp.bfloat16)


def spread(ref, value, tile):
    for k in range(ref.shape[0]):
        ref[k, 0:S] = value[:, :BS]
        ref[k, S : 2 * S] = value[:, BS:]
        ref[k, 2 * S : 2 * S + TILE] = tile


def solve(matrix, right):
    joined = jnp.concatenate([matrix, right], axis=1)
    row = lax.broadcasted_iota(jnp.int32, joined.shape, 0)

    def step(i, x, column):
        pivot = x[i : i + 1, :] / column[i : i + 1, :]
        return jnp.where(row == i, pivot, x - column * pivot)

    for first in range(0, S, GROUP):
        last = first + GROUP
        columns = {
            j: jnp.broadcast_to(joined[:, j : j + 1], joined.shape) for j in range(first, last)
        }
        for i in range(first, last):
            joined = step(i, joined, columns[i])
            for j in range(i + 1, last):
                columns[j] = step(i, columns[j], columns[i])
    return joined[:, S:]


def mix(vectors, small):
    return dot(small.T, vectors)


def grams(left, right):
    return dot(left, right, ((1,), (1,)))


def pack(products, sums=()):
    lane = lax.broadcasted_iota(jnp.int32, (TILE, 2 * S), 1)
    row = lax.broadcasted_iota(jnp.int32, (TILE, 2 * S), 0)
    rest = jnp.zeros((TILE, 2 * S), F32)
    for k, value in enumerate(sums):
        rest = jnp.where((row == 0) & (lane == k), value, rest)
    return jnp.concatenate([products[:TILE], products[TILE:], rest, rest], axis=1)


def unpack(tile):
    whole = jnp.concatenate([tile[:, : 2 * S], tile[:, 2 * S : 4 * S]], axis=0)
    return whole[:, :S], whole[:, S:], tile[:, 4 * S :]


def total(ref, first=0, last=None):
    value = ref[0, first:last]
    for k in range(1, ref.shape[0]):
        value = value + ref[k, first:last]
    image = jnp.concatenate([value[0:S], value[S : 2 * S]], axis=1)
    return image, value[2 * S :]


def entire(x):
    return jnp.sum(jnp.sum(x, axis=1, keepdims=True), axis=0, keepdims=True)


def fetch(blocks, held, done):
    copies = [pltpu.make_async_copy(blocks.at[i], held.at[i], done.at[i]) for i in range(16)]
    for copy in copies:
        copy.start()
    return copies


def prepare_body(source, counts, packed, blocks, done):
    copies = fetch(source, blocks, done)
    for i in range(16):
        copies[i].wait()
        for k in range(2):
            keep = (k < counts[0, i]).astype(F32)
            high, low = halves((blocks[i, k] * keep).T)
            packed[i, k * BS : (k + 1) * BS, 0:BS] = high
            packed[i, k * BS : (k + 1) * BS, BS : 2 * BS] = low


def product_body(own, peer, packed, cols, core, out):
    me = core[0]
    for i in range(16):
        picked = []
        for k in range(2):
            col = cols[k, i]
            m = col >> 2
            b = pl.multiple_of((col & 1) * S, S)
            here = own[m, pl.ds(b, S), :]
            there = peer[m, pl.ds(b, S), :]
            picked.append(jnp.where((col >> 1) & 1 == me, here, there))
        high, low = halves(jnp.concatenate(picked, axis=1))
        result = bdot(jnp.concatenate([high, low], axis=0), packed[i])
        result = (result[:S, :BS] + result[:S, BS:]) + (result[S:, :BS] + result[S:, BS:])
        out[i // 2, (i % 2) * S : (i % 2 + 1) * S] = result
    if own.shape[1] > 2 * S:
        tile, tile2 = own[0, 2 * S :], peer[0, 2 * S :]
        for m in range(1, 16):
            tile = tile + own[m, 2 * S :]
            tile2 = tile2 + peer[m, 2 * S :]
        for c in range(8):
            out[c, 2 * S :] = tile + tile2


def start_body(source, message, shadow, done):
    copy = pltpu.make_async_copy(source, shadow, done)
    copy.start()
    copy.wait()
    value = shadow[...]
    for k in range(message.shape[0]):
        message[k, 0:S] = value[:, :BS]
        message[k, S:] = value[:, BS:]


def first_body(parts, shadow, diag, image, message):
    value, _ = total(parts)
    s = shadow[...]
    v = value + diag[...] * s
    image[...] = v
    spread(message, v, pack(grams(s, jnp.concatenate([v, s], axis=0))))


def lead_step(parts, diag, image, forward, residual):
    value, tile = total(parts)
    v = image[...]
    z = value + diag[...] * v
    matrix, right, _ = unpack(tile)
    alpha = solve(matrix, right)
    q = residual[...] - mix(v, alpha)
    t = forward[...] - mix(z, alpha)
    return matrix, alpha, z, q, t


def lead_body(
    parts, shadow, diag, image, forward, residual, z_out, q_out, t_out, alpha_out, matrix_out, message
):
    matrix, alpha, z, q, t = lead_step(parts, diag, image, forward, residual)
    z_out[...] = z
    q_out[...] = q
    t_out[...] = t
    alpha_out[...] = alpha
    matrix_out[...] = matrix
    products = grams(shadow[...], jnp.concatenate([t, t], axis=0))
    spread(message, t, pack(products, (entire(t * t), entire(t * q))))


def lead_rest_body(matrix, alpha, direction, *rest):
    solution, (inverse_out, x_out) = rest[:-2], rest[-2:]
    row = lax.broadcasted_iota(jnp.int32, (S, S), 0)
    col = lax.broadcasted_iota(jnp.int32, (S, S), 1)
    inverse_out[...] = solve(matrix[...], (row == col).astype(F32))
    x = mix(direction[...], alpha[...])
    x_out[...] = x + solution[0][...] if solution else x


def follow_body(
    parts, shadow, diag, image, z, q, t, inverse, v_out, f_out, r_out, beta_out, omega_out, message
):
    value, tile = total(parts)
    middle = t[...]
    f = value + diag[...] * middle
    cross, _, sums = unpack(tile)
    omega = sums[0:1, 1:2] / sums[0:1, 0:1]
    beta = -dot(inverse[...], cross)
    residual = q[...] - omega * middle
    y = f + mix(z[...], beta)
    image_new = (middle + mix(image[...], beta)) - omega * y
    v_out[...] = image_new
    f_out[...] = f
    r_out[...] = residual
    beta_out[...] = beta
    omega_out[...] = jnp.broadcast_to(omega, omega_out.shape)
    products = grams(shadow[...], jnp.concatenate([image_new, residual], axis=0))
    spread(message, image_new, pack(products))


def follow_rest_body(t, f, r, beta, omega, image, direction, q, x, forward_out, p_out, x_out):
    o = omega[0:1, 0:1]
    forward_out[...] = t[...] - o * f[...]
    p_out[...] = r[...] + mix(direction[...] - o * image[...], beta[...])
    x_out[...] = x[...] + o * q[...]


def last_body(parts, diag, image, forward, residual, q_out, alpha_out, sums):
    _, alpha, _, q, t = lead_step(parts, diag, image, forward, residual)
    q_out[...] = q
    alpha_out[...] = alpha
    lane = lax.broadcasted_iota(jnp.int32, (1, BS), 1)
    sums[...] = jnp.where(lane == 0, entire(t * t), jnp.where(lane == 1, entire(t * q), 0.0))


def end_body(sums, alpha, direction, x, q, out):
    value = jnp.sum(sums[...], axis=0, keepdims=True)
    omega = value[0:1, 1:2] / value[0:1, 0:1]
    out[...] = x[...] + mix(direction[...], alpha[...]) + omega * q[...]


def per_device(rhs, diagonal, blocks, block_cols, counts):
    core = lax.axis_index("core").astype(jnp.int32).reshape(1)
    block_cols = block_cols.T
    counts = counts.T
    shadow = rhs.T
    diag = diagonal.reshape(1, 2 * BS)
    vec = sds(S, 2 * BS)
    small = sds(S, S)
    message = sds(16, 2 * S + TILE, BS)

    def among(x):
        return lax.all_to_all(x, ("x", "z"), 0, 0, tiled=True)

    def across(x):
        return lax.all_to_all(x, "cols", 0, 0, tiled=True)

    def exchange(own):
        return lax.ppermute(own, "core", [(0, 1), (1, 0)])

    def product(own, peer):
        out = call(
            product_body, sds(8, own.shape[1], BS), [VMEM, VMEM, VMEM, SMEM, SMEM],
            own, peer, packed, block_cols, core,
        )
        return across(out)

    held = [pltpu.VMEM((16, 2, BS, BS), F32), pltpu.SemaphoreType.DMA((16,))]
    msg = call(
        start_body, jax.ShapeDtypeStruct((16, 2 * S, BS), F32), [HBM], shadow,
        scratch=[pltpu.VMEM((S, 2 * BS), F32), pltpu.SemaphoreType.DMA],
    )
    own = among(msg)
    packed = call(
        prepare_body, sds(16, 2 * BS, 2 * BS, dtype=jnp.bfloat16), [HBM, SMEM],
        blocks, counts, scratch=held,
    )
    parts = product(own, exchange(own))
    v, msg = call(first_body, (vec, message), [VMEM] * 3, parts, shadow, diag)
    f, r, p, x = v, shadow, shadow, ()
    own = among(msg)
    parts = product(own, exchange(own))
    for _ in range(1, ITERS):
        z, q, t, alpha, matrix, msg = call(
            lead_body, (vec, vec, vec, small, small, message), [VMEM] * 6,
            parts, shadow, diag, v, f, r,
        )
        own = among(msg)
        peer = exchange(own)
        inverse, x = call(lead_rest_body, (small, vec), [VMEM] * (3 + len(x)), matrix, alpha, p, *x)
        parts = product(own, peer)
        image = v
        v, half, r, beta, omega, msg = call(
            follow_body, (vec, vec, vec, small, sds(1, BS), message), [VMEM] * 8,
            parts, shadow, diag, image, z, q, t, inverse,
        )
        own = among(msg)
        peer = exchange(own)
        f, p, x = call(
            follow_rest_body, (vec, vec, vec), [VMEM] * 9,
            t, half, r, beta, omega, image, p, q, x,
        )
        parts = product(own, peer)
        x = (x,)
    q, alpha, sums = call(last_body, (vec, small, sds(1, BS)), [VMEM] * 5, parts, diag, v, f, r)
    everyone = 2 * 16 * 8
    sums = jnp.broadcast_to(sums[None], (everyone, 1, BS))
    sums = lax.all_to_all(sums, ("x", "z", "core", "cols"), 0, 0, tiled=True)
    out = call(
        end_body, jax.ShapeDtypeStruct((S, 2 * BS), F32), [VMEM] * 5, sums.reshape(everyone, BS), alpha, p, x[0], q
    )
    return out.T


def solution(mesh):
    parts = ("x", "z", "core")
    mesh = jax.sharding.Mesh(mesh.devices.reshape(2, 8, 2, 8), (*parts, "cols"))
    in_specs = (
        P((*parts, "cols"), None),
        P((*parts, "cols")),
        P(parts, "cols", None, None),
        P(parts, "cols"),
        P(parts, "cols"),
    )
    out_specs = P((*parts, "cols"), None)
    return jax.shard_map(
        per_device, mesh=mesh, in_specs=in_specs, out_specs=out_specs, check_vma=False
    )
```
